32 devices in a mesh: ctx: 4 (over y, core), exp: 8 (over z, x).
Axes of the slice: x: 2, y: 2, z: 4, core: 2. Of those that a mesh axis runs over, the one named last changes fastest.
Arguments:
- queries: bfloat16 [512, 64, 576], P('ctx', 'exp'), may hold values from -1024 to 1024
- latents: bfloat16 [512, 576], P('ctx'), may hold values from -6.1 to 6.1
- block_starts: int32 [8], replicated, may hold values from 0 to 448, as said below
- w_uv: bfloat16 [64, 512, 128], P('exp'), may hold values from -0.25 to 0.25
- moe_tokens: bfloat16 [1024, 7168], P('exp'), may hold values from -6 to 6
- expert_ids: int32 [1024, 2], P('exp'), may hold values from 0 to 7, as said below
- gate_weights: float32 [1024, 2], P('exp'), may hold values from 0.2 to 1
- w_gate: bfloat16 [8, 7168, 512], P('exp', None, 'ctx'), may hold values from -0.0625 to 0.0625
- w_up: bfloat16 [8, 7168, 512], P('exp', None, 'ctx'), may hold values from -0.0625 to 0.0625
- w_down: bfloat16 [8, 512, 7168], P('exp', 'ctx'), may hold values from -0.25 to 0.25
Outputs:
- attended: bfloat16 [512, 64, 128], P('ctx', 'exp')
- moe_out: bfloat16 [1024, 7168], P('exp', 'ctx')
The draws below stay inside these ranges and needn't reach their ends.
Inputs may be any that keep to these rules, and one draw needn't show every extreme that they name: Token t has position block_starts[t // 64] + t % 64; block_starts is a permutation of the multiples of 64 below 512. `expert_ids`: each row names 2 different experts. In the rows of one index of exp, one expert, the same for every index, is named by exactly 48 rows, no expert by more, and the other experts' counts differ by at most one.
All inputs are finite; a program needn't handle non-finite values.
Results may differ from the reference program's by a relative error of at most 0.018.
Values may be sent and summed in bfloat16 or wider, within the bound.
A program may use at most 128 MiB of HBM per device.

```python
import math
import jax
import jax.numpy as jnp
from jax import lax

D = 7168
LAT = 512
ROPE = 64
VDIM = 128
F_DEV = 128
S_DEV = 128
MT_DEV = 128
TOP = 2
HEADS = 64
FF = 512
TOKENS_A = 512
MT_TOK = 1024
EXPERTS = 8
CAP = 48
N_CTX = 4
N_EXP = 8


def block_order(key):
    return jax.random.permutation(jax.random.fold_in(key, 11), 2 * TOKENS_A // S_DEV).astype(jnp.int32)


def draw_block_starts(key, part):
    return (block_order(key) * (S_DEV // 2)).astype(jnp.int32)


def base_latents(key):
    drawn = jax.random.normal(jax.random.fold_in(key, 12), (TOKENS_A, LAT + ROPE), jnp.float32)
    return jnp.clip(drawn, -6.0, 6.0)


def draw_latents(key, part):
    base = base_latents(key)
    return base.astype(jnp.bfloat16)


def draw_queries(key, part):
    base = jax.random.normal(jax.random.fold_in(key, 13), (TOKENS_A, HEADS, LAT + ROPE), jnp.float32)
    base = jnp.clip(base, -6.0, 6.0)
    return base.astype(jnp.bfloat16)


def draw_expert_ids(key, part):
    full = jax.random.randint(jax.random.fold_in(key, 21), (), 0, EXPERTS)
    column = jnp.arange(TOP, dtype=jnp.int32)[None, :]

    def one_block(block_index):
        inner = jax.random.fold_in(key, 100 + block_index)
        ranking = jax.random.permutation(jax.random.fold_in(inner, 1), MT_DEV).astype(jnp.int32)[:, None]
        offset = jax.random.randint(jax.random.fold_in(inner, 2), (), 0, EXPERTS - 1)
        leading = ranking < CAP
        sequence = jnp.where(leading, ranking * (TOP - 1) + column - 1, CAP * (TOP - 1) + (ranking - CAP) * TOP + column)
        others = (sequence + offset) % (EXPERTS - 1)
        others = others + (others >= full).astype(jnp.int32)
        return jnp.where(leading & (column == 0), full, others).astype(jnp.int32)
    blocks = jax.vmap(one_block)(jnp.arange(MT_TOK // MT_DEV, dtype=jnp.int32))
    return blocks.reshape(MT_TOK, TOP).astype(jnp.int32)


def levels(stream_key, extent, shards, least, high):
    def one(axis_at, parts):
        draws = jax.random.uniform(jax.random.fold_in(jax.random.fold_in(stream_key, 6), axis_at), (parts,), jnp.float32, least / len(shards), high / len(shards))
        return jnp.repeat(jnp.exp(draws), extent[axis_at] // parts).reshape((-1,) + (1,) * (len(extent) - axis_at - 1))

    factor_of = one(*shards[0])
    for cut in shards[1:]:
        factor_of = factor_of * one(*cut)
    return factor_of


def noise(key, dims, spread, reach, split=(), held_as=jnp.bfloat16):
    level = levels(key, dims, split, -0.22, 0.18) if split else 1.0
    entries = jax.random.normal(key, dims, jnp.float32) * spread * level
    return jnp.minimum(jnp.maximum(entries, -reach), reach).astype(held_as)


def setup_inputs(seed: int = 0) -> dict:
    splits = jax.random.split(jax.random.key(seed), 11)
    return {
        "queries": draw_queries(jax.random.fold_in(splits[10], 71), 0),
        "latents": draw_latents(jax.random.fold_in(splits[10], 71), 0),
        "block_starts": draw_block_starts(jax.random.fold_in(splits[10], 71), 0),
        "w_uv": noise(splits[3], (HEADS, LAT, VDIM), LAT ** -0.5, 0.25, ((0, 8),)),
        "moe_tokens": noise(splits[4], (MT_TOK, D), 1.0, 6.0, ((0, 8),)),
        "expert_ids": draw_expert_ids(jax.random.fold_in(splits[10], 71), 0),
        "gate_weights": jnp.clip(0.2 + 0.8 * jax.random.uniform(splits[6], (MT_TOK, TOP), jnp.float32) ** levels(splits[6], (MT_TOK, TOP), ((0, 8),), -0.2, 0.2), 0.2, 1.0),
        "w_gate": noise(splits[7], (EXPERTS, D, FF), D ** -0.5, 0.0625, ((0, 8), (2, 4))),
        "w_up": noise(splits[8], (EXPERTS, D, FF), D ** -0.5, 0.0625, ((0, 8), (2, 4))),
        "w_down": noise(splits[9], (EXPERTS, FF, D), FF ** -0.5, 0.25, ((0, 8), (1, 4))),
    }


score_scale = (0.1 * math.log(40.0) + 1.0) ** 2 / math.sqrt(192.0)
neg_fill = -1e+30

def token_positions(block_starts, token_index, half_block):
    block_index = token_index // half_block
    matches = block_index[:, None] == jnp.arange(block_starts.shape[0], dtype=jnp.int32)[None, :]
    first_pos = lax.optimization_barrier(jnp.sum(jnp.where(matches, block_starts[None, :], 0), axis=1))
    return (first_pos + token_index % half_block).astype(jnp.int32)

def slot_targets(expert_ids, expert_count, capacity):
    token_count, picks = expert_ids.shape
    flat_ids = expert_ids.reshape(token_count * picks)
    onehot = (flat_ids[:, None] == jnp.arange(expert_count, dtype=jnp.int32)[None, :]).astype(jnp.int32)
    earlier = jnp.cumsum(onehot, axis=0) - onehot
    slot_index = lax.optimization_barrier(jnp.sum(earlier * onehot, axis=1))
    return (flat_ids * capacity + slot_index).astype(jnp.int32)

def reference(queries, latents, block_starts, w_uv, moe_tokens, expert_ids, gate_weights, w_gate, w_up, w_down):
    positions = token_positions(block_starts, jnp.arange(TOKENS_A, dtype=jnp.int32), S_DEV // 2)
    visible = positions[None, :] <= positions[:, None]
    values = latents[:, :LAT]

    def one_head(pieces):
        head_queries, head_uv = pieces
        scores = jnp.dot(head_queries, latents.T, preferred_element_type=jnp.float32) * score_scale
        masked = jnp.where(visible, scores, neg_fill)
        top_score = lax.optimization_barrier(jnp.max(masked, axis=1, keepdims=True))
        weights = jnp.where(visible, jnp.exp(masked - top_score), 0.0)
        totals = lax.optimization_barrier(jnp.sum(weights, axis=1, keepdims=True))
        blended = jnp.dot(weights.astype(jnp.bfloat16), values, preferred_element_type=jnp.float32)
        latent_out = (blended / totals).astype(jnp.bfloat16)
        return jnp.dot(latent_out, head_uv, preferred_element_type=jnp.float32).astype(jnp.bfloat16)
    per_head = lax.map(one_head, (jnp.transpose(queries, (1, 0, 2)), w_uv))
    attended = jnp.transpose(per_head, (1, 0, 2))
    block_ids = expert_ids.reshape(N_EXP, MT_DEV, TOP)
    targets = jax.vmap(lambda ids: slot_targets(ids, EXPERTS, CAP))(block_ids)
    local_rows = jnp.arange(MT_DEV * TOP, dtype=jnp.int32) // TOP
    global_rows = jnp.arange(N_EXP, dtype=jnp.int32)[:, None] * MT_DEV + local_rows[None, :]

    def fill_block(target_row, token_row, gate_row):
        filled = jnp.zeros((EXPERTS * CAP,), jnp.int32).at[target_row].set(token_row + 1)
        scaled = jnp.zeros((EXPERTS * CAP,), jnp.float32).at[target_row].set(gate_row)
        return (filled, scaled)
    filled, scaled = jax.vmap(fill_block)(targets, global_rows, gate_weights.reshape(N_EXP, MT_DEV * TOP))
    filled = jnp.transpose(filled.reshape(N_EXP, EXPERTS, CAP), (1, 0, 2)).reshape(EXPERTS, N_EXP * CAP)
    scaled = jnp.transpose(scaled.reshape(N_EXP, EXPERTS, CAP), (1, 0, 2)).reshape(EXPERTS, N_EXP * CAP)

    def one_expert(accum, pieces):
        slot_rows, slot_gates, gate_matrix, up_matrix, down_matrix = pieces
        occupied = slot_rows > 0
        source = jnp.where(occupied, slot_rows - 1, 0)
        inputs = jnp.where(occupied[:, None], moe_tokens[source], 0)
        gate_h = jnp.dot(inputs, gate_matrix, preferred_element_type=jnp.float32)
        up_h = jnp.dot(inputs, up_matrix, preferred_element_type=jnp.float32)
        hidden = (jax.nn.silu(gate_h) * up_h).astype(jnp.bfloat16)

        def add_group(group_index, summed):
            begin = (group_index * F_DEV).astype(jnp.int32)
            hidden_part = lax.dynamic_slice_in_dim(hidden, begin, F_DEV, 1)
            down_part = lax.dynamic_slice_in_dim(down_matrix, begin, F_DEV, 0)
            rounded = jnp.dot(hidden_part, down_part, preferred_element_type=jnp.float32).astype(jnp.bfloat16)
            return summed + lax.optimization_barrier(rounded).astype(jnp.float32)
        summed = lax.fori_loop(0, N_CTX, add_group, jnp.zeros((N_EXP * CAP, D), jnp.float32))
        contrib = jnp.where(occupied[:, None], slot_gates[:, None] * summed, 0.0)
        return (accum.at[source].add(contrib), None)
    accum, _ = lax.scan(one_expert, jnp.zeros((MT_TOK, D), jnp.float32), (filled, scaled, w_gate, w_up, w_down))
    return (attended, accum.astype(jnp.bfloat16))
```

```python
import functools
import math

import jax
import jax.numpy as jnp
from jax import lax
from jax.experimental import pallas as pl
from jax.experimental.pallas import tpu as pltpu
from jax.sharding import PartitionSpec as P

score_scale = (0.1 * math.log(40.0) + 1.0) ** 2 / math.sqrt(192.0)
neg_fill = -1e30


def token_positions(block_starts, token_index, half_block):
    block_index = token_index // half_block
    matches = block_index[:, None] == jnp.arange(block_starts.shape[0], dtype=jnp.int32)[None, :]
    first_pos = jnp.sum(jnp.where(matches, block_starts[None, :], 0), axis=1)
    return first_pos + token_index % half_block


def slot_targets(expert_ids, expert_count, capacity):
    token_count, picks = expert_ids.shape
    flat_ids = expert_ids.reshape(token_count * picks)
    onehot = (flat_ids[:, None] == jnp.arange(expert_count, dtype=jnp.int32)[None, :]).astype(
        jnp.int32
    )
    earlier = jnp.cumsum(onehot, axis=0) - onehot
    slot_index = jnp.sum(earlier * onehot, axis=1)
    return flat_ids * capacity + slot_index


def attention(queries, latents, block_starts, w_uv):
    query_tokens, head_count, entry_width = queries.shape
    lat_width = w_uv.shape[1]
    half_block = query_tokens // 2
    row_total = query_tokens * head_count
    flat_queries = queries.reshape(row_total, entry_width)
    own_index = lax.axis_index("ctx") * query_tokens + jnp.arange(query_tokens, dtype=jnp.int32)
    own_positions = token_positions(block_starts, own_index, half_block)
    query_positions = jnp.repeat(own_positions, head_count)
    shard_piece = lax.all_gather(latents, "ctx", axis=0, tiled=True)
    key_positions = token_positions(
        block_starts, jnp.arange(shard_piece.shape[0], dtype=jnp.int32), half_block
    )
    top_score = jnp.full((row_total,), neg_fill, jnp.float32)
    scores = (
        lax.dot_general(
            flat_queries, shard_piece, (((1,), (1,)), ((), ())), preferred_element_type=jnp.float32
        )
        * score_scale
    )
    visible = key_positions[None, :] <= query_positions[:, None]
    masked = jnp.where(visible, scores, neg_fill)
    new_top = jnp.maximum(top_score, jnp.max(masked, axis=1))
    weights = jnp.where(visible, jnp.exp(masked - new_top[:, None]), 0.0)
    totals = jnp.sum(weights, axis=1)
    blended = jnp.dot(
        weights.astype(jnp.bfloat16), shard_piece[:, :lat_width], preferred_element_type=jnp.float32
    )
    top_score, totals, blended = (new_top, totals, blended)
    latent_out = (
        (blended / totals[:, None])
        .astype(jnp.bfloat16)
        .reshape(query_tokens, head_count, lat_width)
    )
    attended = jnp.einsum(
        "shl,hlv->shv", latent_out, w_uv, preferred_element_type=jnp.float32
    ).astype(jnp.bfloat16)
    return attended


def routed_plain(moe_tokens, expert_ids, gate_weights, w_gate, w_up, w_down):
    token_count, picks = expert_ids.shape
    model_width = moe_tokens.shape[1]
    expert_count = lax.axis_size("exp")
    capacity = 3 * token_count * picks // (2 * expert_count)
    targets = slot_targets(expert_ids, expert_count, capacity)
    source_row = jnp.arange(token_count * picks, dtype=jnp.int32) // picks
    filled = jnp.zeros((expert_count * capacity,), jnp.int32).at[targets].set(source_row + 1)
    occupied = filled > 0
    gate_matrix = w_gate[0]
    up_matrix = w_up[0]
    down_matrix = w_down[0]
    picked_rows = moe_tokens[jnp.where(occupied, filled - 1, 0)]
    outgoing = jnp.where(occupied[:, None], picked_rows, 0).reshape(
        expert_count, capacity, model_width
    )
    arrived = lax.all_to_all(outgoing, "exp", split_axis=0, concat_axis=0, tiled=True)
    senders, slot_count, width_in = arrived.shape
    flat_rows = arrived.reshape(senders * slot_count, width_in)
    gate_h = jnp.dot(flat_rows, gate_matrix, preferred_element_type=jnp.float32)
    up_h = jnp.dot(flat_rows, up_matrix, preferred_element_type=jnp.float32)
    hidden = (jax.nn.silu(gate_h) * up_h).astype(jnp.bfloat16)
    rounded = jnp.dot(hidden, down_matrix, preferred_element_type=jnp.float32).astype(jnp.bfloat16)
    rounded = lax.optimization_barrier(rounded.reshape(senders, slot_count, width_in))
    summed = lax.psum_scatter(
        rounded.astype(jnp.float32).astype(jnp.bfloat16), "ctx", scatter_dimension=2, tiled=True
    ).astype(jnp.float32)
    returned = lax.all_to_all(
        summed.astype(jnp.bfloat16), "exp", split_axis=0, concat_axis=0, tiled=True
    ).astype(summed.dtype)
    out_width = returned.shape[2]
    gathered = returned.reshape(expert_count * capacity, out_width)[targets].reshape(
        token_count, picks, out_width
    )
    weighted = jnp.sum(gathered * gate_weights[:, :, None], axis=1)
    return weighted.astype(jnp.bfloat16)


def flip_bits(index, bits):
    flipped = index
    for bit in range(bits.bit_length()):
        if (bits >> bit) % 2:
            flipped = flipped + (1 << bit) * (1 - 2 * ((index // (1 << bit)) % 2))
    return flipped


def plan(count, heads):
    half = count // 2
    near, far = list(range(1, half)), list(range(half, count))
    left = list(range(heads))
    order = [("compute", 0), ("latents", 0)]

    def attend(share):
        for _ in range(min(share, len(left))):
            order.append(("attend", left.pop(0)))

    attend(2)
    lags = (("forward", 0), ("pass_on", 1), ("compute", 1), ("down", 2))
    for at in range(len(far) + 2):
        if at < len(near):
            order.append(("forward", near[at]))
        if at < len(far):
            order.append(("forward", far[at]))
            order.append(("weights", at))
        if at < len(near):
            order.append(("compute", near[at]))
        if at == 1:
            attend(1)
        if 1 <= at <= len(far):
            order.append(("pass_on", far[at - 1]))
            attend(2)
            order.append(("compute", far[at - 1]))
        if at >= 2:
            order.append(("down", far[at - 2]))
            if at - 2 < len(near):
                order.append(("down", near[at - 2]))
    order.append(("down", 0))
    attend(len(left))
    return order


def dot_first(left, right):
    return lax.dot_general(
        left, right, (((0,), (0,)), ((), ())), preferred_element_type=jnp.float32
    )


def dot_f32(left, right):
    return jnp.dot(left, right, preferred_element_type=jnp.float32)


down_parts = 2


def window_kernel(
    count, capacity, wide, ids_hbm, gates_hbm, latents_hbm, tokens_hbm, starts_hbm, gate_hbm, up_hbm,
    down_hbm, queries_hbm, uv_hbm, out_ref, attended_ref,
    ids, gates, latents, tokens, starts, pair_w, down_w, query_t, uv_w, every_latent, keys, value_t, seen, place, gate_of,
    outgoing, arrived, hidden, back_send, returned,
    load_sem, lat_s, lat_r, out_s, out_r, side_s, side_r, near_s, near_r, relay_s, relay_r,
    hid_s, hid_r, wd_s, wd_r, back_s, back_r,
):
    me = lax.axis_index("exp")
    ctx = lax.axis_index("ctx")
    core = ctx % 2
    other_core = ctx + 1 - 2 * core
    other_row = (ctx + 2) % 4
    opposite = (other_core + 2) % 4
    peers = (other_core, other_row, opposite)
    width = outgoing.shape[3]
    token_count = tokens.shape[0]
    group = down_hbm.shape[1]
    part = group // down_parts
    fan = gate_hbm.shape[2]

    def columns(at):
        return pl.ds(pl.multiple_of(at * width, 128), width)

    inputs = [
        pltpu.make_async_copy(source, target, load_sem.at[5 + at])
        for at, (source, target) in enumerate(
            [(ids_hbm, ids), (tokens_hbm, tokens), (latents_hbm, latents), (gates_hbm, gates),
             (starts_hbm, starts)]
        )
    ]
    for load in inputs:
        load.start()
    loads = [
        pltpu.make_async_copy(gate_hbm.at[0], pair_w.at[:, pl.ds(0, fan)], load_sem.at[0]),
        pltpu.make_async_copy(up_hbm.at[0], pair_w.at[:, pl.ds(fan, fan)], load_sem.at[1]),
        pltpu.make_async_copy(queries_hbm, query_t, load_sem.at[3]),
        pltpu.make_async_copy(uv_hbm, uv_w, load_sem.at[4]),
        pltpu.make_async_copy(down_hbm.at[0, :, columns(ctx)], down_w.at[ctx], load_sem.at[2]),
    ]
    for load in loads:
        load.start()

    barrier = pltpu.get_barrier_semaphore()
    for k in range(1, count):
        pl.semaphore_signal(
            barrier, inc=1, device_id={"exp": flip_bits(me, k), "ctx": ctx},
            device_id_type=pl.DeviceIdType.MESH,
        )
    for peer in peers:
        pl.semaphore_signal(
            barrier, inc=1, device_id={"exp": me, "ctx": peer},
            device_id_type=pl.DeviceIdType.MESH,
        )

    def remote(source, target, send, recv, exp, ctx_at):
        return pltpu.make_async_remote_copy(
            src_ref=source, dst_ref=target, send_sem=send, recv_sem=recv,
            device_id={"exp": exp, "ctx": ctx_at}, device_id_type=pl.DeviceIdType.MESH,
        )

    def quarters(k):
        return (ctx, other_row) if k in wide else (ctx,)

    def dispatch(k):
        to = flip_bits(me, k)
        return [
            remote(
                outgoing.at[k, i], arrived.at[quarter, me], out_s.at[k, i], out_r.at[k, i], to, ctx
            )
            for i, quarter in enumerate(quarters(k))
        ]

    def across(k):
        block = arrived.at[ctx, flip_bits(me, k)]
        return remote(block, block, side_s.at[k], side_r.at[k], me, other_row)

    def beside(k):
        return [
            remote(
                arrived.at[quarter, flip_bits(me, k)], arrived.at[quarter, flip_bits(me, k)],
                near_s.at[k, i], near_r.at[k, i], me, other_core,
            )
            for i, quarter in enumerate(quarters(k))
        ]

    def relay(k):
        block = arrived.at[other_row, flip_bits(me, k)]
        return remote(block, block, relay_s.at[k], relay_r.at[k], me, other_core)

    def share_hidden(k):
        block = hidden.at[k, ctx]
        return [
            remote(block, block, hid_s.at[k, i], hid_r.at[k, i], me, peer)
            for i, peer in enumerate(peers)
        ]

    def share_down(i, piece):
        rows = pl.ds(piece * part, part)
        return remote(
            down_hbm.at[0, rows, columns(peers[i])], down_w.at[ctx, rows],
            wd_s.at[i, piece], wd_r.at[i, piece], me, peers[i],
        )

    def give_back(k):
        to = flip_bits(me, k)
        return remote(
            back_send.at[k], returned.at[me], back_s.at[k], back_r.at[k], to, ctx
        )

    def own_latents(step, peer):
        return remote(
            latents, every_latent.at[ctx], lat_s.at[step], lat_r.at[step], me, peer
        )

    row_block = every_latent.at[other_row]
    latents_beside = own_latents(0, other_core)
    latents_across = own_latents(1, other_row)
    latents_relay = remote(row_block, row_block, lat_s.at[2], lat_r.at[2], me, other_core)

    inputs[0].wait()
    inputs[3].wait()
    expert_at = lax.broadcasted_iota(jnp.int32, (count, token_count), 0)
    first, second = ids[0:1, :] == expert_at, ids[1:2, :] == expert_at
    member = first | second
    before = lax.broadcasted_iota(jnp.int32, (token_count, token_count), 0)
    after = lax.broadcasted_iota(jnp.int32, (token_count, token_count), 1)
    earlier = dot_f32(
        member.astype(jnp.float32).astype(jnp.bfloat16),
        (before < after).astype(jnp.float32).astype(jnp.bfloat16),
    )
    place[...] = jnp.where(member, earlier, -1.0)
    gate_of[...] = jnp.where(first, gates[0:1, :], 0.0) + jnp.where(second, gates[1:2, :], 0.0)
    slot_at = lax.broadcasted_iota(jnp.int32, (capacity, token_count), 0).astype(jnp.float32)

    def chosen(expert):
        return (place[pl.ds(expert, 1), :] == slot_at).astype(jnp.float32).astype(jnp.bfloat16)

    half = count // 2
    far, near = list(range(half, count)), list(range(1, half))

    def select(ks, i, column):
        picks = jnp.concatenate([chosen(flip_bits(me, k)) for k in ks], axis=0)
        rows = dot_f32(picks, tokens[:, columns(column)]).astype(jnp.bfloat16)
        for at, k in enumerate(ks):
            outgoing[k, i] = rows[at * capacity : (at + 1) * capacity]

    inputs[1].wait()
    select(far, 0, ctx)
    inputs[2].wait()
    pl.semaphore_wait(barrier, count + 2)
    latents_across.start()
    latents_beside.start()
    share_down(0, 0).start()
    for piece in range(1, down_parts):
        share_down(0, piece).start()
    for k in far:
        for copy in dispatch(k):
            copy.start()
    share_down(1, 0).start()
    share_down(2, 0).start()
    select(near, 0, ctx)
    if wide:
        select(list(wide), 1, other_row)
    for k in near:
        for copy in dispatch(k):
            copy.start()
    every_latent[ctx] = latents[...]
    mine = chosen(me)
    for quarter in range(4):
        span = pl.ds(quarter * width, width)
        arrived[quarter, me] = dot_f32(mine, tokens[:, span]).astype(jnp.bfloat16)

    span_tokens = latents.shape[1]
    half_block = span_tokens // 2
    lat_width = uv_w.shape[1]

    def gather_latents(_):
        latents_across.wait_recv()
        latents_relay.start()
        inputs[4].wait()
        key_at = lax.broadcasted_iota(jnp.int32, (4 * span_tokens, span_tokens), 0)
        own_at = lax.broadcasted_iota(jnp.int32, (4 * span_tokens, span_tokens), 1)
        key_block = key_at // half_block
        key_start = jnp.zeros_like(key_at)
        for block in range(8):
            key_start = jnp.where(key_block == block, starts[block], key_start)
        own_start = jnp.where(own_at < half_block, starts[2 * ctx], starts[2 * ctx + 1])
        key_position = key_start + key_at % half_block
        seen[...] = (key_position <= own_start + own_at % half_block).astype(jnp.float32)
        latents_beside.wait_recv()
        latents_relay.wait_recv()
        for block in range(4):
            span = pl.ds(block * span_tokens, span_tokens)
            value_t[:, span] = every_latent[block, :lat_width, :]
            keys[span, :] = every_latent[block].T
        for load in loads[2:4]:
            load.wait()

    def attend(head):
        scores = dot_f32(keys[...], query_t[head]) * score_scale
        visible = seen[...] > 0.5
        masked = jnp.where(visible, scores, neg_fill)
        top = jnp.max(masked, axis=0, keepdims=True)
        weights = jnp.where(visible, jnp.exp(masked - top), 0.0)
        totals = jnp.sum(weights, axis=0, keepdims=True)
        blended = dot_f32(value_t[...], weights.astype(jnp.bfloat16))
        latent_out = (blended / totals).astype(jnp.bfloat16)
        attended_ref[head] = dot_first(latent_out, uv_w[head]).astype(jnp.bfloat16)

    def forward(k):
        for copy in dispatch(k):
            copy.wait_recv()
        if k not in wide:
            across(k).start()
        for copy in beside(k):
            copy.start()

    def weights(at):
        piece = at + 1
        if piece < down_parts:
            share_down(1, piece).start()
            share_down(2, piece).start()

    def pass_on(k):
        if k not in wide:
            across(k).wait_recv()
            relay(k).start()

    def compute(k):
        if k:
            for copy in beside(k):
                copy.wait_recv()
            if k not in wide:
                relay(k).wait_recv()
        else:
            loads[0].wait()
            loads[1].wait()
        at = flip_bits(me, k)
        both = jnp.zeros((capacity, 2 * fan), jnp.float32)
        for quarter in range(4):
            both += dot_f32(arrived[quarter, at], pair_w[pl.ds(quarter * width, width), :])
        gate_h, up_h = both[:, :fan], both[:, fan:]
        hidden[k, ctx] = (gate_h / (1.0 + jnp.exp(-gate_h)) * up_h).astype(jnp.bfloat16)
        for copy in share_hidden(k):
            copy.start()

    waiting = [loads[4]]

    def down(k):
        while waiting:
            waiting.pop().wait()
            for i in range(3):
                for piece in range(down_parts):
                    share_down(i, piece).wait_recv()
        for copy in share_hidden(k):
            copy.wait_recv()
        total = dot_f32(hidden[k, 0], down_w[0])
        for block in range(1, 4):
            total += dot_f32(hidden[k, block], down_w[block])
        if k:
            back_send[k] = total.astype(jnp.bfloat16)
            give_back(k).start()
        else:
            returned[me] = total.astype(jnp.bfloat16)

    stages = {
        "forward": forward, "pass_on": pass_on, "compute": compute, "down": down,
        "attend": attend, "latents": gather_latents, "weights": weights,
    }
    for stage, at in plan(count, query_t.shape[0]):
        stages[stage](at)

    spread = jnp.concatenate(
        [
            jnp.where(place[e : e + 1, :] == slot_at, gate_of[e : e + 1, :], 0.0)
            for e in range(count)
        ],
        axis=0,
    )
    high = spread.astype(jnp.bfloat16)
    low = (spread - high.astype(jnp.float32)).astype(jnp.bfloat16)
    for k in range(1, count):
        give_back(k).wait_recv()
    back = returned[...].reshape(count * capacity, width)
    out_ref[...] = (dot_first(high, back) + dot_first(low, back)).astype(jnp.bfloat16)
    for copy in (latents_across, latents_beside, latents_relay):
        copy.wait_send()
    for i in range(3):
        for piece in range(down_parts):
            share_down(i, piece).wait_send()
    for k in range(count):
        copies = share_hidden(k)
        if k:
            copies += dispatch(k) + beside(k) + [give_back(k)]
            if k not in wide:
                copies += [across(k), relay(k)]
        for copy in copies:
            copy.wait_send()


def window_fused(
    queries, latents, block_starts, w_uv, moe_tokens, expert_ids, gate_weights, w_gate, w_up, w_down
):
    queries = jnp.transpose(queries, (1, 2, 0))
    heads, entry_width, query_tokens = queries.shape
    lat_width, value_width = w_uv.shape[1:]
    ways = lax.axis_size("ctx")
    key_count = ways * query_tokens
    token_count, picks = expert_ids.shape
    model_width = moe_tokens.shape[1]
    fan = w_gate.shape[2]
    count = lax.axis_size("exp")
    width = model_width // ways
    capacity = 3 * token_count * picks // (2 * count)
    wide = tuple(range(1, count // 2))
    vmem = pl.BlockSpec(memory_space=pltpu.VMEM)
    hbm = pl.BlockSpec(memory_space=pltpu.HBM)
    block = (capacity, width)
    dtype = jnp.bfloat16
    dma = pltpu.SemaphoreType.DMA
    routed, attended = pl.pallas_call(
        functools.partial(window_kernel, count, capacity, wide),
        out_shape=(
            jax.ShapeDtypeStruct((token_count, width), dtype),
            jax.ShapeDtypeStruct((heads, query_tokens, value_width), dtype),
        ),
        in_specs=[hbm] * 10,
        out_specs=(vmem, vmem),
        scratch_shapes=[
            pltpu.VMEM((picks, token_count), jnp.int32),
            pltpu.VMEM((picks, token_count), jnp.float32),
            pltpu.VMEM((entry_width, query_tokens), dtype),
            pltpu.VMEM((token_count, model_width), dtype),
            pltpu.SMEM(block_starts.shape, jnp.int32),
            pltpu.VMEM((model_width, 2 * fan), dtype),
            pltpu.VMEM((ways, fan, width), dtype),
            pltpu.VMEM(queries.shape, dtype),
            pltpu.VMEM(w_uv.shape, dtype),
            pltpu.VMEM((ways, entry_width, query_tokens), dtype),
            pltpu.VMEM((key_count, entry_width), dtype),
            pltpu.VMEM((lat_width, key_count), dtype),
            pltpu.VMEM((key_count, query_tokens), jnp.float32),
            pltpu.VMEM((count, token_count), jnp.float32),
            pltpu.VMEM((count, token_count), jnp.float32),
            pltpu.VMEM((count, 2) + block, dtype),
            pltpu.VMEM((ways, count) + block, dtype),
            pltpu.VMEM((count, ways, capacity, fan), dtype),
            pltpu.VMEM((count,) + block, dtype),
            pltpu.VMEM((count,) + block, dtype),
            dma((10,)), dma((3,)), dma((3,)),
            dma((count, 2)), dma((count, 2)),
            dma((count,)), dma((count,)),
            dma((count, 2)), dma((count, 2)),
            dma((count,)), dma((count,)),
            dma((count, 3)), dma((count, 3)),
            dma((3, down_parts)), dma((3, down_parts)),
            dma((count,)), dma((count,)),
        ],
        compiler_params=pltpu.CompilerParams(
            collective_id=0, has_side_effects=True, vmem_limit_bytes=40 * 1024 * 1024
        ),
    )(
        *[
            pltpu.with_memory_space_constraint(operand, pltpu.HBM)
            for operand in (
                expert_ids.T, gate_weights.T, latents.T, moe_tokens, block_starts,
                w_gate, w_up, w_down, queries, w_uv,
            )
        ]
    )
    return jnp.transpose(attended, (1, 0, 2)), routed


def shards(
    queries, latents, block_starts, w_uv, moe_tokens, expert_ids, gate_weights, w_gate, w_up, w_down
):
    count = lax.axis_size("exp")
    ways = lax.axis_size("ctx")
    token_count, picks = expert_ids.shape
    capacity = 3 * token_count * picks // (2 * count)
    fits = ways == 4 and count & (count - 1) == 0 and count >= 4 and capacity % 16 == 0
    fits = fits and moe_tokens.shape[1] % (128 * ways) == 0 and block_starts.shape[0] == 8
    fits = fits and picks == 2 and w_gate.shape[2] % 128 == 0
    if fits:
        return window_fused(
            queries, latents, block_starts, w_uv, moe_tokens, expert_ids, gate_weights,
            w_gate, w_up, w_down,
        )
    attended = attention(queries, latents, block_starts, w_uv)
    return attended, routed_plain(moe_tokens, expert_ids, gate_weights, w_gate, w_up, w_down)


def solution(mesh):
    in_specs = (
        P("ctx", "exp", None),
        P("ctx", None),
        P(),
        P("exp", None, None),
        P("exp", None),
        P("exp", None),
        P("exp", None),
        P("exp", None, "ctx"),
        P("exp", None, "ctx"),
        P("exp", "ctx", None),
    )
    out_specs = (P("ctx", "exp", None), P("exp", "ctx"))
    return jax.shard_map(shards, mesh=mesh, in_specs=in_specs, out_specs=out_specs, check_vma=False)
```

```python
import functools
import math

import jax
import jax.numpy as jnp
from jax import lax
from jax.experimental import pallas as pl
from jax.experimental.pallas import tpu as pltpu
from jax.sharding import PartitionSpec as P

score_scale = (0.1 * math.log(40.0) + 1.0) ** 2 / math.sqrt(192.0)
neg_fill = -1e30


def token_positions(block_starts, token_index, half_block):
    block_index = token_index // half_block
    matches = block_index[:, None] == jnp.arange(block_starts.shape[0], dtype=jnp.int32)[None, :]
    first_pos = jnp.sum(jnp.where(matches, block_starts[None, :], 0), axis=1)
    return first_pos + token_index % half_block


def slot_targets(expert_ids, expert_count, capacity):
    token_count, picks = expert_ids.shape
    flat_ids = expert_ids.reshape(token_count * picks)
    onehot = (flat_ids[:, None] == jnp.arange(expert_count, dtype=jnp.int32)[None, :]).astype(
        jnp.int32
    )
    earlier = jnp.cumsum(onehot, axis=0) - onehot
    slot_index = jnp.sum(earlier * onehot, axis=1)
    return flat_ids * capacity + slot_index


def attention(queries, latents, block_starts, w_uv):
    query_tokens, head_count, entry_width = queries.shape
    lat_width = w_uv.shape[1]
    half_block = query_tokens // 2
    row_total = query_tokens * head_count
    flat_queries = queries.reshape(row_total, entry_width)
    own_index = lax.axis_index("ctx") * query_tokens + jnp.arange(query_tokens, dtype=jnp.int32)
    own_positions = token_positions(block_starts, own_index, half_block)
    query_positions = jnp.repeat(own_positions, head_count)
    shard_piece = lax.all_gather(latents, "ctx", axis=0, tiled=True)
    key_positions = token_positions(
        block_starts, jnp.arange(shard_piece.shape[0], dtype=jnp.int32), half_block
    )
    top_score = jnp.full((row_total,), neg_fill, jnp.float32)
    scores = (
        lax.dot_general(
            flat_queries, shard_piece, (((1,), (1,)), ((), ())), preferred_element_type=jnp.float32
        )
        * score_scale
    )
    visible = key_positions[None, :] <= query_positions[:, None]
    masked = jnp.where(visible, scores, neg_fill)
    new_top = jnp.maximum(top_score, jnp.max(masked, axis=1))
    weights = jnp.where(visible, jnp.exp(masked - new_top[:, None]), 0.0)
    totals = jnp.sum(weights, axis=1)
    blended = jnp.dot(
        weights.astype(jnp.bfloat16), shard_piece[:, :lat_width], preferred_element_type=jnp.float32
    )
    top_score, totals, blended = (new_top, totals, blended)
    latent_out = (
        (blended / totals[:, None])
        .astype(jnp.bfloat16)
        .reshape(query_tokens, head_count, lat_width)
    )
    attended = jnp.einsum(
        "shl,hlv->shv", latent_out, w_uv, preferred_element_type=jnp.float32
    ).astype(jnp.bfloat16)
    return attended


def routed_plain(moe_tokens, expert_ids, gate_weights, w_gate, w_up, w_down):
    token_count, picks = expert_ids.shape
    model_width = moe_tokens.shape[1]
    expert_count = lax.axis_size("exp")
    capacity = 3 * token_count * picks // (2 * expert_count)
    targets = slot_targets(expert_ids, expert_count, capacity)
    source_row = jnp.arange(token_count * picks, dtype=jnp.int32) // picks
    filled = jnp.zeros((expert_count * capacity,), jnp.int32).at[targets].set(source_row + 1)
    occupied = filled > 0
    gate_matrix = w_gate[0]
    up_matrix = w_up[0]
    down_matrix = w_down[0]
    picked_rows = moe_tokens[jnp.where(occupied, filled - 1, 0)]
    outgoing = jnp.where(occupied[:, None], picked_rows, 0).reshape(
        expert_count, capacity, model_width
    )
    arrived = lax.all_to_all(outgoing, "exp", split_axis=0, concat_axis=0, tiled=True)
    senders, slot_count, width_in = arrived.shape
    flat_rows = arrived.reshape(senders * slot_count, width_in)
    gate_h = jnp.dot(flat_rows, gate_matrix, preferred_element_type=jnp.float32)
    up_h = jnp.dot(flat_rows, up_matrix, preferred_element_type=jnp.float32)
    hidden = (jax.nn.silu(gate_h) * up_h).astype(jnp.bfloat16)
    rounded = jnp.dot(hidden, down_matrix, preferred_element_type=jnp.float32).astype(jnp.bfloat16)
    rounded = lax.optimization_barrier(rounded.reshape(senders, slot_count, width_in))
    summed = lax.psum_scatter(
        rounded.astype(jnp.float32).astype(jnp.bfloat16), "ctx", scatter_dimension=2, tiled=True
    ).astype(jnp.float32)
    returned = lax.all_to_all(
        summed.astype(jnp.bfloat16), "exp", split_axis=0, concat_axis=0, tiled=True
    ).astype(summed.dtype)
    out_width = returned.shape[2]
    gathered = returned.reshape(expert_count * capacity, out_width)[targets].reshape(
        token_count, picks, out_width
    )
    weighted = jnp.sum(gathered * gate_weights[:, :, None], axis=1)
    return weighted.astype(jnp.bfloat16)


def flip_bits(index, bits):
    flipped = index
    for bit in range(bits.bit_length()):
        if (bits >> bit) % 2:
            flipped = flipped + (1 << bit) * (1 - 2 * ((index // (1 << bit)) % 2))
    return flipped


down_parts = 1


def plan(count, heads):
    half = count // 2
    near, far = list(range(1, half)), list(range(half, count))
    order = [("compute", 0)]
    order += [("forward", k) for k in near[:-1]]
    order += [("compute", k) for k in near[:-1]]
    order += [("forward", far[0]), ("forward", near[-1]), ("compute", near[-1])]
    order += [("down", 0)] + [("down", k) for k in near[:-1]]
    order += [("forward", far[1]), ("pass_on", far[0]), ("down", near[-1]), ("compute", far[0])]
    order += [("forward", far[2])]
    for at in range(1, len(far)):
        order += [("pass_on", far[at]), ("down", far[at - 1]), ("compute", far[at])]
        if at + 2 < len(far):
            order += [("forward", far[at + 2])]
        elif at + 2 == len(far):
            order += [("latents", 0)]
    order += [("gather", 0), ("down", far[-1])]
    order += [("attend", 0), ("attend", 2), ("settle", 0)]
    order += [("attend", head) for head in range(4, heads, 2)]
    return order


def dot_first(left, right):
    return lax.dot_general(
        left, right, (((0,), (0,)), ((), ())), preferred_element_type=jnp.float32
    )


def dot_f32(left, right):
    return jnp.dot(left, right, preferred_element_type=jnp.float32)


def window_kernel(
    count, capacity, base, wide, ids_hbm, gates_hbm, latents_hbm, tokens_hbm, starts_hbm, gate_hbm, up_hbm,
    down_hbm, queries_hbm, uv_hbm, out_ref, attended_ref,
    ids, gates, latents, tokens, starts, pair_w, down_w, query_t, uv_w, every_latent, keys, value_t, seen, place, gate_of,
    outgoing, far_rows, arrived, hidden, back_send, collected, settled, returned,
    load_sem, lat_s, lat_r, out_s, out_r, side_s, side_r, near_s, near_r, relay_s, relay_r,
    hid_s, hid_r, wd_s, wd_r, back_s, back_r, fan_s, fan_r, collect_s, collect_r, settle_s, settle_r,
):
    me = lax.axis_index("exp")
    ctx = lax.axis_index("ctx")
    core = ctx % 2
    other_core = ctx + 1 - 2 * core
    other_row = (ctx + 2) % 4
    opposite = (other_core + 2) % 4
    peers = (other_core, other_row, opposite)
    width = outgoing.shape[3]
    token_count = tokens.shape[0]
    group = down_hbm.shape[1]
    part = group // down_parts
    fan = gate_hbm.shape[2]

    def columns(at):
        return pl.ds(pl.multiple_of(at * width, 128), width)

    inputs = [
        pltpu.make_async_copy(source, target, load_sem.at[5 + at])
        for at, (source, target) in enumerate(
            [(ids_hbm, ids), (tokens_hbm, tokens), (latents_hbm, latents), (gates_hbm, gates),
             (starts_hbm, starts)]
        )
    ]
    for load in inputs:
        load.start()
    loads = [
        pltpu.make_async_copy(gate_hbm.at[0], pair_w.at[:, pl.ds(0, fan)], load_sem.at[0]),
        pltpu.make_async_copy(up_hbm.at[0], pair_w.at[:, pl.ds(fan, fan)], load_sem.at[1]),
        pltpu.make_async_copy(queries_hbm, query_t, load_sem.at[3]),
        pltpu.make_async_copy(uv_hbm, uv_w, load_sem.at[4]),
        pltpu.make_async_copy(down_hbm.at[0, :, columns(ctx)], down_w.at[ctx], load_sem.at[2]),
    ]
    for load in loads:
        load.start()

    barrier = pltpu.get_barrier_semaphore()
    for k in range(1, count):
        pl.semaphore_signal(
            barrier, inc=1, device_id={"exp": flip_bits(me, k), "ctx": ctx},
            device_id_type=pl.DeviceIdType.MESH,
        )
    for peer in peers:
        pl.semaphore_signal(
            barrier, inc=1, device_id={"exp": me, "ctx": peer},
            device_id_type=pl.DeviceIdType.MESH,
        )

    def remote(source, target, send, recv, exp, ctx_at):
        return pltpu.make_async_remote_copy(
            src_ref=source, dst_ref=target, send_sem=send, recv_sem=recv,
            device_id={"exp": exp, "ctx": ctx_at}, device_id_type=pl.DeviceIdType.MESH,
        )

    half = count // 2
    rest = capacity - base
    far, near = list(range(half, count)), list(range(1, half))

    def far_start(k):
        return (k - half) * base + (rest if k > half else 0)

    def rows_of(k):
        return base if k > half else capacity

    def slots(k):
        if k < half:
            return pl.ds(k * capacity, capacity)
        return pl.ds(half * capacity + (k - half) * base, base)

    extra_slots = pl.ds(half * (capacity + base), rest)
    low_rows, high_rows = pl.ds(0, base), pl.ds(base, rest)

    def quarters(k):
        return (ctx, other_row) if k in wide else (ctx,)

    def dispatch(k):
        to = flip_bits(me, k)
        if k >= half:
            rows = rows_of(k)
            source = far_rows.at[pl.ds(far_start(k), rows)]
            target = arrived.at[ctx, me, pl.ds(0, rows)]
            return [remote(source, target, out_s.at[k, 0], out_r.at[k, 0], to, ctx)]
        return [
            remote(
                outgoing.at[k, i], arrived.at[quarter, me], out_s.at[k, i], out_r.at[k, i], to, ctx
            )
            for i, quarter in enumerate(quarters(k))
        ]

    def fan_out(k):
        block = arrived.at[ctx, flip_bits(me, half), high_rows]
        return remote(block, block, fan_s.at[k], fan_r.at[k], flip_bits(me, k), ctx)

    def across(k):
        block = arrived.at[ctx, flip_bits(me, k)]
        return remote(block, block, side_s.at[k], side_r.at[k], me, other_row)

    def beside(k):
        return [
            remote(
                arrived.at[quarter, flip_bits(me, k)], arrived.at[quarter, flip_bits(me, k)],
                near_s.at[k, i], near_r.at[k, i], me, other_core,
            )
            for i, quarter in enumerate(quarters(k))
        ]

    def relay(k):
        block = arrived.at[other_row, flip_bits(me, k)]
        return remote(block, block, relay_s.at[k], relay_r.at[k], me, other_core)

    def share_hidden(k):
        block = hidden.at[k, ctx]
        return [
            remote(block, block, hid_s.at[k, i], hid_r.at[k, i], me, peer)
            for i, peer in enumerate(peers)
        ]

    def share_down(i, piece):
        rows = pl.ds(piece * part, part)
        return remote(
            down_hbm.at[0, rows, columns(peers[i])], down_w.at[ctx, rows],
            wd_s.at[i, piece], wd_r.at[i, piece], me, peers[i],
        )

    def give_back(k):
        to = flip_bits(me, k)
        source = back_send.at[k, low_rows] if k >= half else back_send.at[k]
        return remote(source, returned.at[slots(k)], back_s.at[k], back_r.at[k], to, ctx)

    def collect(k):
        return remote(
            back_send.at[k + half, high_rows], collected.at[k], collect_s.at[k], collect_r.at[k],
            flip_bits(me, k), ctx,
        )

    def settle_extra():
        return remote(
            settled, returned.at[extra_slots], settle_s.at[0], settle_r.at[0],
            flip_bits(me, half), ctx,
        )

    def own_latents(step, peer):
        return remote(
            latents, every_latent.at[ctx], lat_s.at[step], lat_r.at[step], me, peer
        )

    row_block = every_latent.at[other_row]
    latents_beside = own_latents(0, other_core)
    latents_across = own_latents(1, other_row)
    latents_relay = remote(row_block, row_block, lat_s.at[2], lat_r.at[2], me, other_core)

    inputs[0].wait()
    inputs[3].wait()
    expert_at = lax.broadcasted_iota(jnp.int32, (count, token_count), 0)
    first, second = ids[0:1, :] == expert_at, ids[1:2, :] == expert_at
    member = first | second
    before = lax.broadcasted_iota(jnp.int32, (token_count, token_count), 0)
    after = lax.broadcasted_iota(jnp.int32, (token_count, token_count), 1)
    earlier = dot_f32(
        member.astype(jnp.float32).astype(jnp.bfloat16),
        (before < after).astype(jnp.float32).astype(jnp.bfloat16),
    )
    place[...] = jnp.where(member, earlier, -1.0)
    gate_of[...] = jnp.where(first, gates[0:1, :], 0.0) + jnp.where(second, gates[1:2, :], 0.0)
    slot_at = lax.broadcasted_iota(jnp.int32, (capacity, token_count), 0).astype(jnp.float32)

    def row_of(ref, k):
        return ref[pl.ds(flip_bits(me, k), 1), :]

    def one_hot(k, first_slot, last_slot):
        return (row_of(place, k) == slot_at[first_slot:last_slot]).astype(jnp.float32)

    def take(picks, column):
        rows = dot_f32(picks.astype(jnp.bfloat16), tokens[:, columns(column)])
        return rows.astype(jnp.bfloat16)

    def select(ks, i, column):
        rows = take(jnp.concatenate([one_hot(k, 0, capacity) for k in ks], axis=0), column)
        for at, k in enumerate(ks):
            outgoing[k, i] = rows[at * capacity : (at + 1) * capacity]

    def select_far():
        picks = [one_hot(k, 0, base) for k in far]
        extra = one_hot(half, base, capacity)
        for k in far[1:]:
            extra += one_hot(k, base, capacity)
        far_rows[...] = take(jnp.concatenate(picks[:1] + [extra] + picks[1:], axis=0), ctx)

    inputs[1].wait()
    select(near, 0, ctx)
    if wide:
        select(list(wide), 1, other_row)
    inputs[2].wait()
    pl.semaphore_wait(barrier, count + 2)
    for k in near:
        for copy in dispatch(k):
            copy.start()
    for i in (1, 2, 0):
        for piece in range(down_parts):
            share_down(i, piece).start()
    latents_beside.start()
    select_far()
    for k in far:
        for copy in dispatch(k):
            copy.start()
    every_latent[ctx] = latents[...]
    mine = one_hot(0, 0, capacity).astype(jnp.bfloat16)
    for quarter in range(4):
        span = pl.ds(quarter * width, width)
        arrived[quarter, me] = dot_f32(mine, tokens[:, span]).astype(jnp.bfloat16)

    span_tokens = latents.shape[1]
    half_block = span_tokens // 2
    lat_width = uv_w.shape[1]

    def send_latents(_):
        latents_across.start()

    def gather_latents(_):
        latents_across.wait_recv()
        latents_relay.start()
        inputs[4].wait()
        key_at = lax.broadcasted_iota(jnp.int32, (4 * span_tokens, span_tokens), 0)
        own_at = lax.broadcasted_iota(jnp.int32, (4 * span_tokens, span_tokens), 1)
        key_block = key_at // half_block
        key_start = jnp.zeros_like(key_at)
        for block in range(8):
            key_start = jnp.where(key_block == block, starts[block], key_start)
        own_start = jnp.where(own_at < half_block, starts[2 * ctx], starts[2 * ctx + 1])
        key_position = key_start + key_at % half_block
        seen[...] = (key_position <= own_start + own_at % half_block).astype(jnp.float32)
        latents_beside.wait_recv()
        latents_relay.wait_recv()
        for block in range(4):
            span = pl.ds(block * span_tokens, span_tokens)
            value_t[:, span] = every_latent[block, :lat_width, :]
            keys[span, :] = every_latent[block].T
        for load in loads[2:4]:
            load.wait()

    def attend(head):
        pair = range(head, min(head + 2, query_t.shape[0]))
        wide_query = jnp.concatenate([query_t[at] for at in pair], axis=1)
        visible = jnp.concatenate([seen[...] for _ in pair], axis=1) > 0.5
        scores = dot_f32(keys[...], wide_query) * score_scale
        masked = jnp.where(visible, scores, neg_fill)
        top = jnp.max(masked, axis=0, keepdims=True)
        weights = jnp.where(visible, jnp.exp(masked - top), 0.0)
        totals = jnp.sum(weights, axis=0, keepdims=True)
        blended = dot_f32(value_t[...], weights.astype(jnp.bfloat16))
        latent_out = (blended / totals).astype(jnp.bfloat16)
        for spot, at in enumerate(pair):
            span = slice(spot * span_tokens, (spot + 1) * span_tokens)
            attended_ref[at] = dot_first(latent_out[:, span], uv_w[at]).astype(jnp.bfloat16)

    def forward(k):
        for copy in dispatch(k):
            copy.wait_recv()
        if k == half:
            for other in near:
                fan_out(other).start()
        elif k > half:
            fan_out(k - half).wait_recv()
        if k not in wide:
            across(k).start()
        for copy in beside(k):
            copy.start()

    def pass_on(k):
        if k not in wide:
            across(k).wait_recv()
            relay(k).start()

    def compute(k):
        if k:
            for copy in beside(k):
                copy.wait_recv()
            if k not in wide:
                relay(k).wait_recv()
        else:
            loads[0].wait()
            loads[1].wait()
        at = flip_bits(me, k)
        both = jnp.zeros((capacity, 2 * fan), jnp.float32)
        for quarter in range(4):
            both += dot_f32(arrived[quarter, at], pair_w[pl.ds(quarter * width, width), :])
        gate_h, up_h = both[:, :fan], both[:, fan:]
        hidden[k, ctx] = (gate_h / (1.0 + jnp.exp(-gate_h)) * up_h).astype(jnp.bfloat16)
        for copy in share_hidden(k):
            copy.start()

    waiting = [loads[4]]
    is_full = jnp.max(row_of(place, 0), axis=1, keepdims=True) >= float(base)

    def down(k):
        while waiting:
            waiting.pop().wait()
            for i in range(3):
                for piece in range(down_parts):
                    share_down(i, piece).wait_recv()
        for copy in share_hidden(k):
            copy.wait_recv()
        total = dot_f32(hidden[k, 0], down_w[0])
        for block in range(1, 4):
            total += dot_f32(hidden[k, block], down_w[block])
        if k == 0:
            returned[slots(0)] = total.astype(jnp.bfloat16)
            return
        if k >= half:
            back_send[k, low_rows] = total[:base].astype(jnp.bfloat16)
            back_send[k, high_rows] = jnp.where(is_full, total[base:], 0.0).astype(jnp.bfloat16)
        else:
            back_send[k] = total.astype(jnp.bfloat16)
        if k > half:
            collect(k - half).start()
        give_back(k).start()

    def settle(_):
        extra = back_send[half, high_rows].astype(jnp.float32)
        for k in near:
            collect(k).wait_recv()
            extra += collected[k].astype(jnp.float32)
        settled[...] = extra.astype(jnp.bfloat16)
        settle_extra().start()

    stages = {
        "forward": forward, "pass_on": pass_on, "compute": compute, "down": down,
        "attend": attend, "latents": send_latents, "gather": gather_latents,
        "settle": settle,
    }
    for stage, at in plan(count, query_t.shape[0]):
        stages[stage](at)

    def share_of(k, first_slot, last_slot):
        return one_hot(k, first_slot, last_slot) * row_of(gate_of, k)

    extra = share_of(half, base, capacity)
    for k in far[1:]:
        extra += share_of(k, base, capacity)
    spread = jnp.concatenate(
        [share_of(k, 0, capacity) for k in range(half)]
        + [share_of(k, 0, base) for k in far]
        + [extra],
        axis=0,
    )
    high = spread.astype(jnp.bfloat16)
    low = (spread - high.astype(jnp.float32)).astype(jnp.bfloat16)
    for k in range(1, count):
        give_back(k).wait_recv()
    settle_extra().wait_recv()
    back = returned[...]
    out_ref[...] = (dot_first(high, back) + dot_first(low, back)).astype(jnp.bfloat16)
    for copy in (latents_across, latents_beside, latents_relay, settle_extra()):
        copy.wait_send()
    for i in range(3):
        for piece in range(down_parts):
            share_down(i, piece).wait_send()
    for k in range(count):
        copies = share_hidden(k)
        if k:
            copies += dispatch(k) + beside(k) + [give_back(k)]
            if k < half:
                copies += [fan_out(k), collect(k)]
            if k not in wide:
                copies += [across(k), relay(k)]
        for copy in copies:
            copy.wait_send()


def base_rows(row_count, capacity, count):
    spare = -(-(row_count - capacity) // (count - 1))
    return 16 * -(-spare // 16)


def window_fused(
    queries, latents, block_starts, w_uv, moe_tokens, expert_ids, gate_weights, w_gate, w_up, w_down
):
    queries = jnp.transpose(queries, (1, 2, 0))
    heads, entry_width, query_tokens = queries.shape
    lat_width, value_width = w_uv.shape[1:]
    ways = lax.axis_size("ctx")
    key_count = ways * query_tokens
    token_count, picks = expert_ids.shape
    model_width = moe_tokens.shape[1]
    fan = w_gate.shape[2]
    count = lax.axis_size("exp")
    width = model_width // ways
    capacity = 3 * token_count * picks // (2 * count)
    half = count // 2
    wide = tuple(range(1, half))
    base = base_rows(token_count * picks, capacity, count)
    rest = capacity - base
    vmem = pl.BlockSpec(memory_space=pltpu.VMEM)
    hbm = pl.BlockSpec(memory_space=pltpu.HBM)
    block = (capacity, width)
    dtype = jnp.bfloat16
    dma = pltpu.SemaphoreType.DMA
    routed, attended = pl.pallas_call(
        functools.partial(window_kernel, count, capacity, base, wide),
        out_shape=(
            jax.ShapeDtypeStruct((token_count, width), dtype),
            jax.ShapeDtypeStruct((heads, query_tokens, value_width), dtype),
        ),
        in_specs=[hbm] * 10,
        out_specs=(vmem, vmem),
        scratch_shapes=[
            pltpu.VMEM((picks, token_count), jnp.int32),
            pltpu.VMEM((picks, token_count), jnp.float32),
            pltpu.VMEM((entry_width, query_tokens), dtype),
            pltpu.VMEM((token_count, model_width), dtype),
            pltpu.SMEM(block_starts.shape, jnp.int32),
            pltpu.VMEM((model_width, 2 * fan), dtype),
            pltpu.VMEM((ways, fan, width), dtype),
            pltpu.VMEM(queries.shape, dtype),
            pltpu.VMEM(w_uv.shape, dtype),
            pltpu.VMEM((ways, entry_width, query_tokens), dtype),
            pltpu.VMEM((key_count, entry_width), dtype),
            pltpu.VMEM((lat_width, key_count), dtype),
            pltpu.VMEM((key_count, query_tokens), jnp.float32),
            pltpu.VMEM((count, token_count), jnp.float32),
            pltpu.VMEM((count, token_count), jnp.float32),
            pltpu.VMEM((half, 2) + block, dtype),
            pltpu.VMEM((half * base + rest, width), dtype),
            pltpu.VMEM((ways, count) + block, dtype),
            pltpu.VMEM((count, ways, capacity, fan), dtype),
            pltpu.VMEM((count,) + block, dtype),
            pltpu.VMEM((half, rest, width), dtype),
            pltpu.VMEM((rest, width), dtype),
            pltpu.VMEM((half * (capacity + base) + rest, width), dtype),
            dma((10,)), dma((3,)), dma((3,)),
            dma((count, 2)), dma((count, 2)),
            dma((count,)), dma((count,)),
            dma((count, 2)), dma((count, 2)),
            dma((count,)), dma((count,)),
            dma((count, 3)), dma((count, 3)),
            dma((3, down_parts)), dma((3, down_parts)),
            dma((count,)), dma((count,)),
            dma((half,)), dma((half,)),
            dma((half,)), dma((half,)),
            dma((1,)), dma((1,)),
        ],
        compiler_params=pltpu.CompilerParams(
            collective_id=0, has_side_effects=True, vmem_limit_bytes=40 * 1024 * 1024
        ),
    )(
        *[
            pltpu.with_memory_space_constraint(operand, pltpu.HBM)
            for operand in (
                expert_ids.T, gate_weights.T, latents.T, moe_tokens, block_starts,
                w_gate, w_up, w_down, queries, w_uv,
            )
        ]
    )
    return jnp.transpose(attended, (1, 0, 2)), routed


def shards(
    queries, latents, block_starts, w_uv, moe_tokens, expert_ids, gate_weights, w_gate, w_up, w_down
):
    count = lax.axis_size("exp")
    ways = lax.axis_size("ctx")
    token_count, picks = expert_ids.shape
    capacity = 3 * token_count * picks // (2 * count)
    fits = ways == 4 and count & (count - 1) == 0 and count >= 4 and capacity % 16 == 0
    fits = fits and moe_tokens.shape[1] % (128 * ways) == 0 and block_starts.shape[0] == 8
    base = base_rows(token_count * picks, capacity, count)
    fits = fits and base < capacity and count >= 8
    fits = fits and picks == 2 and w_gate.shape[2] % 128 == 0
    if fits:
        return window_fused(
            queries, latents, block_starts, w_uv, moe_tokens, expert_ids, gate_weights,
            w_gate, w_up, w_down,
        )
    attended = attention(queries, latents, block_starts, w_uv)
    return attended, routed_plain(moe_tokens, expert_ids, gate_weights, w_gate, w_up, w_down)


def solution(mesh):
    in_specs = (
        P("ctx", "exp", None),
        P("ctx", None),
        P(),
        P("exp", None, None),
        P("exp", None),
        P("exp", None),
        P("exp", None),
        P("exp", None, "ctx"),
        P("exp", None, "ctx"),
        P("exp", "ctx", None),
    )
    out_specs = (P("ctx", "exp", None), P("exp", "ctx"))
    return jax.shard_map(shards, mesh=mesh, in_specs=in_specs, out_specs=out_specs, check_vma=False)
```

```python
import functools
import math

import jax
import jax.numpy as jnp
from jax import lax
from jax.experimental import pallas as pl
from jax.experimental.pallas import tpu as pltpu
from jax.sharding import PartitionSpec as P

score_scale = (0.1 * math.log(40.0) + 1.0) ** 2 / math.sqrt(192.0)
neg_fill = -1e30


def token_positions(block_starts, token_index, half_block):
    block_index = token_index // half_block
    matches = block_index[:, None] == jnp.arange(block_starts.shape[0], dtype=jnp.int32)[None, :]
    first_pos = jnp.sum(jnp.where(matches, block_starts[None, :], 0), axis=1)
    return first_pos + token_index % half_block


def slot_targets(expert_ids, expert_count, capacity):
    token_count, picks = expert_ids.shape
    flat_ids = expert_ids.reshape(token_count * picks)
    onehot = (flat_ids[:, None] == jnp.arange(expert_count, dtype=jnp.int32)[None, :]).astype(
        jnp.int32
    )
    earlier = jnp.cumsum(onehot, axis=0) - onehot
    slot_index = jnp.sum(earlier * onehot, axis=1)
    return flat_ids * capacity + slot_index


def attention(queries, latents, block_starts, w_uv):
    query_tokens, head_count, entry_width = queries.shape
    lat_width = w_uv.shape[1]
    half_block = query_tokens // 2
    row_total = query_tokens * head_count
    flat_queries = queries.reshape(row_total, entry_width)
    own_index = lax.axis_index("ctx") * query_tokens + jnp.arange(query_tokens, dtype=jnp.int32)
    own_positions = token_positions(block_starts, own_index, half_block)
    query_positions = jnp.repeat(own_positions, head_count)
    shard_piece = lax.all_gather(latents, "ctx", axis=0, tiled=True)
    key_positions = token_positions(
        block_starts, jnp.arange(shard_piece.shape[0], dtype=jnp.int32), half_block
    )
    top_score = jnp.full((row_total,), neg_fill, jnp.float32)
    scores = (
        lax.dot_general(
            flat_queries, shard_piece, (((1,), (1,)), ((), ())), preferred_element_type=jnp.float32
        )
        * score_scale
    )
    visible = key_positions[None, :] <= query_positions[:, None]
    masked = jnp.where(visible, scores, neg_fill)
    new_top = jnp.maximum(top_score, jnp.max(masked, axis=1))
    weights = jnp.where(visible, jnp.exp(masked - new_top[:, None]), 0.0)
    totals = jnp.sum(weights, axis=1)
    blended = jnp.dot(
        weights.astype(jnp.bfloat16), shard_piece[:, :lat_width], preferred_element_type=jnp.float32
    )
    top_score, totals, blended = (new_top, totals, blended)
    latent_out = (
        (blended / totals[:, None])
        .astype(jnp.bfloat16)
        .reshape(query_tokens, head_count, lat_width)
    )
    attended = jnp.einsum(
        "shl,hlv->shv", latent_out, w_uv, preferred_element_type=jnp.float32
    ).astype(jnp.bfloat16)
    return attended


def routed_plain(moe_tokens, expert_ids, gate_weights, w_gate, w_up, w_down):
    token_count, picks = expert_ids.shape
    model_width = moe_tokens.shape[1]
    expert_count = lax.axis_size("exp")
    capacity = 3 * token_count * picks // (2 * expert_count)
    targets = slot_targets(expert_ids, expert_count, capacity)
    source_row = jnp.arange(token_count * picks, dtype=jnp.int32) // picks
    filled = jnp.zeros((expert_count * capacity,), jnp.int32).at[targets].set(source_row + 1)
    occupied = filled > 0
    gate_matrix = w_gate[0]
    up_matrix = w_up[0]
    down_matrix = w_down[0]
    picked_rows = moe_tokens[jnp.where(occupied, filled - 1, 0)]
    outgoing = jnp.where(occupied[:, None], picked_rows, 0).reshape(
        expert_count, capacity, model_width
    )
    arrived = lax.all_to_all(outgoing, "exp", split_axis=0, concat_axis=0, tiled=True)
    senders, slot_count, width_in = arrived.shape
    flat_rows = arrived.reshape(senders * slot_count, width_in)
    gate_h = jnp.dot(flat_rows, gate_matrix, preferred_element_type=jnp.float32)
    up_h = jnp.dot(flat_rows, up_matrix, preferred_element_type=jnp.float32)
    hidden = (jax.nn.silu(gate_h) * up_h).astype(jnp.bfloat16)
    rounded = jnp.dot(hidden, down_matrix, preferred_element_type=jnp.float32).astype(jnp.bfloat16)
    rounded = lax.optimization_barrier(rounded.reshape(senders, slot_count, width_in))
    summed = lax.psum_scatter(
        rounded.astype(jnp.float32).astype(jnp.bfloat16), "ctx", scatter_dimension=2, tiled=True
    ).astype(jnp.float32)
    returned = lax.all_to_all(
        summed.astype(jnp.bfloat16), "exp", split_axis=0, concat_axis=0, tiled=True
    ).astype(summed.dtype)
    out_width = returned.shape[2]
    gathered = returned.reshape(expert_count * capacity, out_width)[targets].reshape(
        token_count, picks, out_width
    )
    weighted = jnp.sum(gathered * gate_weights[:, :, None], axis=1)
    return weighted.astype(jnp.bfloat16)


def flip_bits(index, bits):
    flipped = index
    for bit in range(bits.bit_length()):
        if (bits >> bit) % 2:
            flipped = flipped + (1 << bit) * (1 - 2 * ((index // (1 << bit)) % 2))
    return flipped


down_parts = 4


def far_order(count):
    half = count // 2
    return [half, half + 1] + list(range(count - 1, half + 1, -1))


def plan(count, heads):
    half = count // 2
    near, far = list(range(1, half)), far_order(count)
    last, late = far[-1], near[2:]
    order = [("compute", 0), ("forward", far[0])]
    order += [("send", k) for k in far[2:] + late]
    order += [("weights", down_parts - 1), ("prepare", 0)]
    order += [("forward", k) for k in near[:2]] + [("compute", k) for k in near[:2]]
    order += [("pass_on", far[0]), ("compute", far[0])]
    order += [("forward", far[1]), ("forward", far[2])]
    order += [("gated", k) for k in [0] + near[:2]]
    order += [("down", 0), ("gated", far[0]), ("down", near[0]), ("down", far[0])]
    order += [("pass_on", far[1]), ("down", near[1]), ("compute", far[1])]
    for at in range(2, len(far)):
        k, before = far[at], far[at - 1]
        if at + 1 < len(far):
            order += [("forward", far[at + 1])] + [("forward", other) for other in late]
        order += [("pass_on", k)]
        if k == last:
            order += [("gated", other) for other in late + [before]]
            order += [("compute", k), ("down", before), ("gated", k), ("latents", 0)]
        else:
            order += [("compute", other) for other in late]
            order += [("compute", k), ("gated", before), ("down", before)]
    order += [("down", last)] + [("down", k) for k in late]
    order += [("gather", 0)]
    order += [("attend", head) for head in range(0, heads - 4, 2)]
    order += [("settle", 0), ("attend", heads - 4), ("attend", heads - 2)]
    return order


def dot_first(left, right):
    return lax.dot_general(
        left, right, (((0,), (0,)), ((), ())), preferred_element_type=jnp.float32
    )


def dot_f32(left, right):
    return jnp.dot(left, right, preferred_element_type=jnp.float32)


def window_kernel(
    count, capacity, base, wide, ids_hbm, gates_hbm, latents_hbm, tokens_hbm, starts_hbm, gate_hbm, up_hbm,
    down_hbm, queries_hbm, uv_hbm, out_ref, attended_ref,
    ids, gates, latents, tokens, starts, pair_w, down_w, query_t, uv_w, every_latent, keys, value_t, seen, place, gate_of,
    outgoing, far_rows, arrived, hidden, back_send, collected, settled, returned, share, mixed,
    load_sem, lat_s, lat_r, out_s, out_r, side_s, side_r, near_s, near_r, relay_s, relay_r,
    hid_s, hid_r, wd_s, wd_r, back_s, back_r, fan_s, fan_r, collect_s, collect_r, settle_s, settle_r,
):
    me = lax.axis_index("exp")
    ctx = lax.axis_index("ctx")
    core = ctx % 2
    other_core = ctx + 1 - 2 * core
    other_row = (ctx + 2) % 4
    opposite = (other_core + 2) % 4
    peers = (other_core, other_row, opposite)
    width = outgoing.shape[3]
    token_count = tokens.shape[0]
    group = down_hbm.shape[1]
    part = group // down_parts
    fan = gate_hbm.shape[2]

    def columns(at):
        return pl.ds(pl.multiple_of(at * width, 128), width)

    inputs = [
        pltpu.make_async_copy(source, target, load_sem.at[5 + at])
        for at, (source, target) in enumerate(
            [(ids_hbm, ids), (tokens_hbm, tokens), (latents_hbm, latents), (gates_hbm, gates),
             (starts_hbm, starts)]
        )
    ]
    for load in inputs:
        load.start()
    loads = [
        pltpu.make_async_copy(gate_hbm.at[0], pair_w.at[:, pl.ds(0, fan)], load_sem.at[0]),
        pltpu.make_async_copy(up_hbm.at[0], pair_w.at[:, pl.ds(fan, fan)], load_sem.at[1]),
        pltpu.make_async_copy(queries_hbm, query_t, load_sem.at[3]),
        pltpu.make_async_copy(uv_hbm, uv_w, load_sem.at[4]),
        pltpu.make_async_copy(down_hbm.at[0, :, columns(ctx)], down_w.at[ctx], load_sem.at[2]),
    ]

    barrier = pltpu.get_barrier_semaphore()
    for k in range(1, count):
        pl.semaphore_signal(
            barrier, inc=1, device_id={"exp": flip_bits(me, k), "ctx": ctx},
            device_id_type=pl.DeviceIdType.MESH,
        )
    for peer in peers:
        pl.semaphore_signal(
            barrier, inc=1, device_id={"exp": me, "ctx": peer},
            device_id_type=pl.DeviceIdType.MESH,
        )

    def remote(source, target, send, recv, exp, ctx_at):
        return pltpu.make_async_remote_copy(
            src_ref=source, dst_ref=target, send_sem=send, recv_sem=recv,
            device_id={"exp": exp, "ctx": ctx_at}, device_id_type=pl.DeviceIdType.MESH,
        )

    half = count // 2
    rest = capacity - base
    far, near = list(range(half, count)), list(range(1, half))
    sequence = far_order(count)

    def far_start(k):
        return (k - half) * base + (rest if k > half else 0)

    def rows_of(k):
        return base if k > half else capacity

    def slots(k):
        if k < half:
            return pl.ds(k * capacity, capacity)
        return pl.ds(half * capacity + sequence.index(k) * base, base)

    extra_slots = pl.ds(half * (capacity + base), rest)
    low_rows, high_rows = pl.ds(0, base), pl.ds(base, rest)

    def quarters(k):
        return (ctx, other_row) if k in wide else (ctx,)

    def dispatch(k):
        to = flip_bits(me, k)
        if k >= half:
            rows = rows_of(k)
            source = far_rows.at[pl.ds(far_start(k), rows)]
            target = arrived.at[ctx, me, pl.ds(0, rows)]
            return [remote(source, target, out_s.at[k, 0], out_r.at[k, 0], to, ctx)]
        return [
            remote(
                outgoing.at[k, i], arrived.at[quarter, me], out_s.at[k, i], out_r.at[k, i], to, ctx
            )
            for i, quarter in enumerate(quarters(k))
        ]

    def fan_out(k):
        block = arrived.at[ctx, flip_bits(me, half), high_rows]
        return remote(block, block, fan_s.at[k], fan_r.at[k], flip_bits(me, k), ctx)

    def across(k):
        block = arrived.at[ctx, flip_bits(me, k)]
        return remote(block, block, side_s.at[k], side_r.at[k], me, other_row)

    def beside(k):
        return [
            remote(
                arrived.at[quarter, flip_bits(me, k)], arrived.at[quarter, flip_bits(me, k)],
                near_s.at[k, i], near_r.at[k, i], me, other_core,
            )
            for i, quarter in enumerate(quarters(k))
        ]

    def relay(k):
        block = arrived.at[other_row, flip_bits(me, k)]
        return remote(block, block, relay_s.at[k], relay_r.at[k], me, other_core)

    def share_hidden(k):
        block = hidden.at[k, ctx]
        return [
            remote(block, block, hid_s.at[k, i], hid_r.at[k, i], me, peer)
            for i, peer in enumerate((other_core, other_row))
        ]

    def relay_hidden(k):
        block = hidden.at[k, other_row]
        return remote(block, block, hid_s.at[k, 2], hid_r.at[k, 2], me, other_core)

    def share_down(i, piece):
        rows = pl.ds(piece * part, part)
        return remote(
            down_hbm.at[0, rows, columns(peers[i])], down_w.at[ctx, rows],
            wd_s.at[i, piece], wd_r.at[i, piece], me, peers[i],
        )

    def give_back(k):
        to = flip_bits(me, k)
        source = back_send.at[k, low_rows] if k >= half else back_send.at[k]
        return remote(source, returned.at[slots(k)], back_s.at[k], back_r.at[k], to, ctx)

    def collect(k):
        return remote(
            back_send.at[k + half, high_rows], collected.at[k], collect_s.at[k], collect_r.at[k],
            flip_bits(me, k), ctx,
        )

    def settle_extra():
        return remote(
            settled, returned.at[extra_slots], settle_s.at[0], settle_r.at[0],
            flip_bits(me, half), ctx,
        )

    def own_latents(step, peer):
        return remote(
            latents, every_latent.at[ctx], lat_s.at[step], lat_r.at[step], me, peer
        )

    row_block = every_latent.at[other_row]
    latents_beside = own_latents(0, other_core)
    latents_across = own_latents(1, other_row)
    latents_relay = remote(row_block, row_block, lat_s.at[2], lat_r.at[2], me, other_core)

    pl.semaphore_wait(barrier, count + 2)
    for piece in range(down_parts - 1):
        for i in (1, 2):
            share_down(i, piece).start()
    inputs[0].wait()
    inputs[3].wait()
    expert_at = lax.broadcasted_iota(jnp.int32, (count, token_count), 0)
    first, second = ids[0:1, :] == expert_at, ids[1:2, :] == expert_at
    member = first | second
    before = lax.broadcasted_iota(jnp.int32, (token_count, token_count), 0)
    after = lax.broadcasted_iota(jnp.int32, (token_count, token_count), 1)
    earlier = dot_f32(
        member.astype(jnp.float32).astype(jnp.bfloat16),
        (before < after).astype(jnp.float32).astype(jnp.bfloat16),
    )
    place[...] = jnp.where(member, earlier, -1.0)
    gate_of[...] = jnp.where(first, gates[0:1, :], 0.0) + jnp.where(second, gates[1:2, :], 0.0)
    slot_at = lax.broadcasted_iota(jnp.int32, (capacity, token_count), 0).astype(jnp.float32)

    def row_of(ref, k):
        return ref[pl.ds(flip_bits(me, k), 1), :]

    def one_hot(k, first_slot, last_slot):
        return (row_of(place, k) == slot_at[first_slot:last_slot]).astype(jnp.float32)

    def take(picks, column):
        rows = dot_f32(picks.astype(jnp.bfloat16), tokens[:, columns(column)])
        return rows.astype(jnp.bfloat16)

    def select(ks, i, column):
        rows = take(jnp.concatenate([one_hot(k, 0, capacity) for k in ks], axis=0), column)
        for at, k in enumerate(ks):
            outgoing[k, i] = rows[at * capacity : (at + 1) * capacity]

    def select_far():
        picks = [one_hot(k, 0, base) for k in far]
        extra = one_hot(half, base, capacity)
        for k in far[1:]:
            extra += one_hot(k, base, capacity)
        far_rows[...] = take(jnp.concatenate(picks[:1] + [extra] + picks[1:], axis=0), ctx)

    def send(k):
        for copy in dispatch(k):
            copy.start()

    inputs[1].wait()
    select(near, 0, ctx)
    if wide:
        select(list(wide), 1, other_row)
    send(near[1])
    send(near[0])
    select_far()
    send(sequence[0])
    send(sequence[1])
    for load in loads:
        load.start()
    for piece in range(down_parts):
        share_down(0, piece).start()
    inputs[2].wait()
    latents_beside.start()
    every_latent[ctx] = latents[...]
    mine = one_hot(0, 0, capacity).astype(jnp.bfloat16)
    for quarter in range(4):
        span = pl.ds(quarter * width, width)
        arrived[quarter, me] = dot_f32(mine, tokens[:, span]).astype(jnp.bfloat16)

    span_tokens = latents.shape[1]
    half_block = span_tokens // 2
    lat_width = uv_w.shape[1]

    def send_latents(_):
        latents_across.start()

    def gather_latents(_):
        latents_across.wait_recv()
        latents_relay.start()
        inputs[4].wait()
        key_at = lax.broadcasted_iota(jnp.int32, (4 * span_tokens, span_tokens), 0)
        own_at = lax.broadcasted_iota(jnp.int32, (4 * span_tokens, span_tokens), 1)
        key_block = key_at // half_block
        key_start = jnp.zeros_like(key_at)
        for block in range(8):
            key_start = jnp.where(key_block == block, starts[block], key_start)
        own_start = jnp.where(own_at < half_block, starts[2 * ctx], starts[2 * ctx + 1])
        key_position = key_start + key_at % half_block
        seen[...] = (key_position <= own_start + own_at % half_block).astype(jnp.float32)
        latents_beside.wait_recv()
        latents_relay.wait_recv()
        for block in range(4):
            span = pl.ds(block * span_tokens, span_tokens)
            value_t[:, span] = every_latent[block, :lat_width, :]
            keys[span, :] = every_latent[block].T
        for load in loads[2:4]:
            load.wait()

    def attend(head):
        pair = range(head, min(head + 2, query_t.shape[0]))
        wide_query = jnp.concatenate([query_t[at] for at in pair], axis=1)
        visible = jnp.concatenate([seen[...] for _ in pair], axis=1) > 0.5
        scores = dot_f32(keys[...], wide_query) * score_scale
        masked = jnp.where(visible, scores, neg_fill)
        top = jnp.max(masked, axis=0, keepdims=True)
        weights = jnp.where(visible, jnp.exp(masked - top), 0.0)
        totals = jnp.sum(weights, axis=0, keepdims=True)
        blended = dot_f32(value_t[...], weights.astype(jnp.bfloat16))
        latent_out = (blended / totals).astype(jnp.bfloat16)
        for spot, at in enumerate(pair):
            span = slice(spot * span_tokens, (spot + 1) * span_tokens)
            attended_ref[at] = dot_first(latent_out[:, span], uv_w[at]).astype(jnp.bfloat16)

    def forward(k):
        for copy in dispatch(k):
            copy.wait_recv()
        if k == half:
            for other in sequence[1:]:
                fan_out(other - half).start()
        elif k > half:
            fan_out(k - half).wait_recv()
        if k not in wide:
            across(k).start()
        for copy in beside(k):
            copy.start()

    def weights(piece):
        for i in (1, 2):
            share_down(i, piece).start()

    def pass_on(k):
        if k not in wide:
            across(k).wait_recv()
            relay(k).start()

    def compute(k):
        if k:
            for copy in beside(k):
                copy.wait_recv()
            if k not in wide:
                relay(k).wait_recv()
        else:
            loads[0].wait()
            loads[1].wait()
        at = flip_bits(me, k)
        both = jnp.zeros((capacity, 2 * fan), jnp.float32)
        for quarter in range(4):
            both += dot_f32(arrived[quarter, at], pair_w[pl.ds(quarter * width, width), :])
        gate_h, up_h = both[:, :fan], both[:, fan:]
        hidden[k, ctx] = (gate_h / (1.0 + jnp.exp(-gate_h)) * up_h).astype(jnp.bfloat16)
        for copy in share_hidden(k):
            copy.start()

    waiting = [loads[4]]
    is_full = jnp.max(row_of(place, 0), axis=1, keepdims=True) >= float(base)

    def down(k):
        while waiting:
            waiting.pop().wait()
            for i in range(3):
                for piece in range(down_parts):
                    share_down(i, piece).wait_recv()
        share_hidden(k)[0].wait_recv()
        relay_hidden(k).wait_recv()
        total = dot_f32(hidden[k, 0], down_w[0])
        for block in range(1, 4):
            total += dot_f32(hidden[k, block], down_w[block])
        if k == 0:
            returned[slots(0)] = total.astype(jnp.bfloat16)
            return
        if k >= half:
            back_send[k, low_rows] = total[:base].astype(jnp.bfloat16)
            back_send[k, high_rows] = jnp.where(is_full, total[base:], 0.0).astype(jnp.bfloat16)
        else:
            back_send[k] = total.astype(jnp.bfloat16)
        if k > half:
            collect(k - half).start()
        give_back(k).start()

    def gated(k):
        share_hidden(k)[1].wait_recv()
        relay_hidden(k).start()

    def settle(_):
        extra = back_send[half, high_rows].astype(jnp.float32)
        for k in near:
            collect(k).wait_recv()
            extra += collected[k].astype(jnp.float32)
        settled[...] = extra.astype(jnp.bfloat16)
        settle_extra().start()

    early = half * capacity + (half - 2) * base
    total_rows = half * (capacity + base) + rest

    def prepare(_):
        def share_of(k, first_slot, last_slot):
            return one_hot(k, first_slot, last_slot) * row_of(gate_of, k)

        extra = share_of(half, base, capacity)
        for k in far[1:]:
            extra += share_of(k, base, capacity)
        spread = jnp.concatenate(
            [share_of(k, 0, capacity) for k in range(half)]
            + [share_of(k, 0, base) for k in sequence]
            + [extra],
            axis=0,
        )
        pad = jnp.zeros((share.shape[2] - total_rows, token_count), jnp.float32)
        spread = jnp.concatenate([spread, pad], axis=0).T
        high = spread.astype(jnp.bfloat16)
        share[0] = high
        share[1] = (spread - high.astype(jnp.float32)).astype(jnp.bfloat16)

    def mix(first_row, last_row):
        rows = returned[first_row:last_row]
        high, low = share[0, :, first_row:last_row], share[1, :, first_row:last_row]
        return dot_f32(high, rows) + dot_f32(low, rows)

    stages = {
        "forward": forward, "pass_on": pass_on, "compute": compute, "down": down,
        "attend": attend, "latents": send_latents, "gather": gather_latents, "weights": weights,
        "settle": settle, "prepare": prepare, "send": send, "gated": gated,
    }
    for stage, at in plan(count, query_t.shape[0]):
        stages[stage](at)

    for k in near + sequence[: half - 2]:
        give_back(k).wait_recv()
    mixed[...] = mix(0, early)
    for k in sequence[half - 2 :]:
        give_back(k).wait_recv()
    settle_extra().wait_recv()
    out_ref[...] = (mixed[...] + mix(early, total_rows)).astype(jnp.bfloat16)
    for copy in (latents_across, latents_beside, latents_relay, settle_extra()):
        copy.wait_send()
    for i in range(3):
        for piece in range(down_parts):
            share_down(i, piece).wait_send()
    for k in range(count):
        copies = share_hidden(k) + [relay_hidden(k)]
        if k:
            copies += dispatch(k) + beside(k) + [give_back(k)]
            if k < half:
                copies += [fan_out(k), collect(k)]
            if k not in wide:
                copies += [across(k), relay(k)]
        for copy in copies:
            copy.wait_send()


def base_rows(row_count, capacity, count):
    spare = -(-(row_count - capacity) // (count - 1))
    return 16 * -(-spare // 16)


def window_fused(
    queries, latents, block_starts, w_uv, moe_tokens, expert_ids, gate_weights, w_gate, w_up, w_down
):
    queries = jnp.transpose(queries, (1, 2, 0))
    heads, entry_width, query_tokens = queries.shape
    lat_width, value_width = w_uv.shape[1:]
    ways = lax.axis_size("ctx")
    key_count = ways * query_tokens
    token_count, picks = expert_ids.shape
    model_width = moe_tokens.shape[1]
    fan = w_gate.shape[2]
    count = lax.axis_size("exp")
    width = model_width // ways
    capacity = 3 * token_count * picks // (2 * count)
    half = count // 2
    wide = tuple(range(1, half))
    base = base_rows(token_count * picks, capacity, count)
    rest = capacity - base
    share_width = 128 * -(-(half * (capacity + base) + rest) // 128)
    vmem = pl.BlockSpec(memory_space=pltpu.VMEM)
    hbm = pl.BlockSpec(memory_space=pltpu.HBM)
    block = (capacity, width)
    dtype = jnp.bfloat16
    dma = pltpu.SemaphoreType.DMA
    routed, attended = pl.pallas_call(
        functools.partial(window_kernel, count, capacity, base, wide),
        out_shape=(
            jax.ShapeDtypeStruct((token_count, width), dtype),
            jax.ShapeDtypeStruct((heads, query_tokens, value_width), dtype),
        ),
        in_specs=[hbm] * 10,
        out_specs=(vmem, vmem),
        scratch_shapes=[
            pltpu.VMEM((picks, token_count), jnp.int32),
            pltpu.VMEM((picks, token_count), jnp.float32),
            pltpu.VMEM((entry_width, query_tokens), dtype),
            pltpu.VMEM((token_count, model_width), dtype),
            pltpu.SMEM(block_starts.shape, jnp.int32),
            pltpu.VMEM((model_width, 2 * fan), dtype),
            pltpu.VMEM((ways, fan, width), dtype),
            pltpu.VMEM(queries.shape, dtype),
            pltpu.VMEM(w_uv.shape, dtype),
            pltpu.VMEM((ways, entry_width, query_tokens), dtype),
            pltpu.VMEM((key_count, entry_width), dtype),
            pltpu.VMEM((lat_width, key_count), dtype),
            pltpu.VMEM((key_count, query_tokens), jnp.float32),
            pltpu.VMEM((count, token_count), jnp.float32),
            pltpu.VMEM((count, token_count), jnp.float32),
            pltpu.VMEM((half, 2) + block, dtype),
            pltpu.VMEM((half * base + rest, width), dtype),
            pltpu.VMEM((ways, count) + block, dtype),
            pltpu.VMEM((count, ways, capacity, fan), dtype),
            pltpu.VMEM((count,) + block, dtype),
            pltpu.VMEM((half, rest, width), dtype),
            pltpu.VMEM((rest, width), dtype),
            pltpu.VMEM((half * (capacity + base) + rest, width), dtype),
            pltpu.VMEM((2, token_count, share_width), dtype),
            pltpu.VMEM((token_count, width), jnp.float32),
            dma((10,)), dma((3,)), dma((3,)),
            dma((count, 2)), dma((count, 2)),
            dma((count,)), dma((count,)),
            dma((count, 2)), dma((count, 2)),
            dma((count,)), dma((count,)),
            dma((count, 3)), dma((count, 3)),
            dma((3, down_parts)), dma((3, down_parts)),
            dma((count,)), dma((count,)),
            dma((half,)), dma((half,)),
            dma((half,)), dma((half,)),
            dma((1,)), dma((1,)),
        ],
        compiler_params=pltpu.CompilerParams(
            collective_id=0, has_side_effects=True, vmem_limit_bytes=40 * 1024 * 1024
        ),
    )(
        *[
            pltpu.with_memory_space_constraint(operand, pltpu.HBM)
            for operand in (
                expert_ids.T, gate_weights.T, latents.T, moe_tokens, block_starts,
                w_gate, w_up, w_down, queries, w_uv,
            )
        ]
    )
    return jnp.transpose(attended, (1, 0, 2)), routed


def shards(
    queries, latents, block_starts, w_uv, moe_tokens, expert_ids, gate_weights, w_gate, w_up, w_down
):
    count = lax.axis_size("exp")
    ways = lax.axis_size("ctx")
    token_count, picks = expert_ids.shape
    capacity = 3 * token_count * picks // (2 * count)
    fits = ways == 4 and count & (count - 1) == 0 and count >= 4 and capacity % 16 == 0
    fits = fits and moe_tokens.shape[1] % (128 * ways) == 0 and block_starts.shape[0] == 8
    base = base_rows(token_count * picks, capacity, count)
    fits = fits and base < capacity and count >= 8
    fits = fits and picks == 2 and w_gate.shape[2] % 128 == 0
    if fits:
        return window_fused(
            queries, latents, block_starts, w_uv, moe_tokens, expert_ids, gate_weights,
            w_gate, w_up, w_down,
        )
    attended = attention(queries, latents, block_starts, w_uv)
    return attended, routed_plain(moe_tokens, expert_ids, gate_weights, w_gate, w_up, w_down)


def solution(mesh):
    in_specs = (
        P("ctx", "exp", None),
        P("ctx", None),
        P(),
        P("exp", None, None),
        P("exp", None),
        P("exp", None),
        P("exp", None),
        P("exp", None, "ctx"),
        P("exp", None, "ctx"),
        P("exp", "ctx", None),
    )
    out_specs = (P("ctx", "exp", None), P("exp", "ctx"))
    return jax.shard_map(shards, mesh=mesh, in_specs=in_specs, out_specs=out_specs, check_vma=False)
```

```python
import functools
import math

import jax
import jax.numpy as jnp
from jax import lax
from jax.experimental import pallas as pl
from jax.experimental.pallas import tpu as pltpu
from jax.sharding import PartitionSpec as P

score_scale = (0.1 * math.log(40.0) + 1.0) ** 2 / math.sqrt(192.0)
neg_fill = -1e30


def token_positions(block_starts, token_index, half_block):
    block_index = token_index // half_block
    matches = block_index[:, None] == jnp.arange(block_starts.shape[0], dtype=jnp.int32)[None, :]
    first_pos = jnp.sum(jnp.where(matches, block_starts[None, :], 0), axis=1)
    return first_pos + token_index % half_block


def slot_targets(expert_ids, expert_count, capacity):
    token_count, picks = expert_ids.shape
    flat_ids = expert_ids.reshape(token_count * picks)
    onehot = (flat_ids[:, None] == jnp.arange(expert_count, dtype=jnp.int32)[None, :]).astype(
        jnp.int32
    )
    earlier = jnp.cumsum(onehot, axis=0) - onehot
    slot_index = jnp.sum(earlier * onehot, axis=1)
    return flat_ids * capacity + slot_index


def attention(queries, latents, block_starts, w_uv):
    query_tokens, head_count, entry_width = queries.shape
    lat_width = w_uv.shape[1]
    half_block = query_tokens // 2
    row_total = query_tokens * head_count
    flat_queries = queries.reshape(row_total, entry_width)
    own_index = lax.axis_index("ctx") * query_tokens + jnp.arange(query_tokens, dtype=jnp.int32)
    own_positions = token_positions(block_starts, own_index, half_block)
    query_positions = jnp.repeat(own_positions, head_count)
    shard_piece = lax.all_gather(latents, "ctx", axis=0, tiled=True)
    key_positions = token_positions(
        block_starts, jnp.arange(shard_piece.shape[0], dtype=jnp.int32), half_block
    )
    top_score = jnp.full((row_total,), neg_fill, jnp.float32)
    scores = (
        lax.dot_general(
            flat_queries, shard_piece, (((1,), (1,)), ((), ())), preferred_element_type=jnp.float32
        )
        * score_scale
    )
    visible = key_positions[None, :] <= query_positions[:, None]
    masked = jnp.where(visible, scores, neg_fill)
    new_top = jnp.maximum(top_score, jnp.max(masked, axis=1))
    weights = jnp.where(visible, jnp.exp(masked - new_top[:, None]), 0.0)
    totals = jnp.sum(weights, axis=1)
    blended = jnp.dot(
        weights.astype(jnp.bfloat16), shard_piece[:, :lat_width], preferred_element_type=jnp.float32
    )
    top_score, totals, blended = (new_top, totals, blended)
    latent_out = (
        (blended / totals[:, None])
        .astype(jnp.bfloat16)
        .reshape(query_tokens, head_count, lat_width)
    )
    attended = jnp.einsum(
        "shl,hlv->shv", latent_out, w_uv, preferred_element_type=jnp.float32
    ).astype(jnp.bfloat16)
    return attended


def routed_plain(moe_tokens, expert_ids, gate_weights, w_gate, w_up, w_down):
    token_count, picks = expert_ids.shape
    model_width = moe_tokens.shape[1]
    expert_count = lax.axis_size("exp")
    capacity = 3 * token_count * picks // (2 * expert_count)
    targets = slot_targets(expert_ids, expert_count, capacity)
    source_row = jnp.arange(token_count * picks, dtype=jnp.int32) // picks
    filled = jnp.zeros((expert_count * capacity,), jnp.int32).at[targets].set(source_row + 1)
    occupied = filled > 0
    gate_matrix = w_gate[0]
    up_matrix = w_up[0]
    down_matrix = w_down[0]
    picked_rows = moe_tokens[jnp.where(occupied, filled - 1, 0)]
    outgoing = jnp.where(occupied[:, None], picked_rows, 0).reshape(
        expert_count, capacity, model_width
    )
    arrived = lax.all_to_all(outgoing, "exp", split_axis=0, concat_axis=0, tiled=True)
    senders, slot_count, width_in = arrived.shape
    flat_rows = arrived.reshape(senders * slot_count, width_in)
    gate_h = jnp.dot(flat_rows, gate_matrix, preferred_element_type=jnp.float32)
    up_h = jnp.dot(flat_rows, up_matrix, preferred_element_type=jnp.float32)
    hidden = (jax.nn.silu(gate_h) * up_h).astype(jnp.bfloat16)
    rounded = jnp.dot(hidden, down_matrix, preferred_element_type=jnp.float32).astype(jnp.bfloat16)
    rounded = lax.optimization_barrier(rounded.reshape(senders, slot_count, width_in))
    summed = lax.psum_scatter(
        rounded.astype(jnp.float32).astype(jnp.bfloat16), "ctx", scatter_dimension=2, tiled=True
    ).astype(jnp.float32)
    returned = lax.all_to_all(
        summed.astype(jnp.bfloat16), "exp", split_axis=0, concat_axis=0, tiled=True
    ).astype(summed.dtype)
    out_width = returned.shape[2]
    gathered = returned.reshape(expert_count * capacity, out_width)[targets].reshape(
        token_count, picks, out_width
    )
    weighted = jnp.sum(gathered * gate_weights[:, :, None], axis=1)
    return weighted.astype(jnp.bfloat16)


def flip_bits(index, bits):
    flipped = index
    for bit in range(bits.bit_length()):
        if (bits >> bit) % 2:
            flipped = flipped + (1 << bit) * (1 - 2 * ((index // (1 << bit)) % 2))
    return flipped


down_parts = 4


def far_order(count):
    half = count // 2
    return [half, half + 1] + list(range(count - 1, half + 1, -1))


def plan(count, heads):
    half = count // 2
    near, far = list(range(1, half)), far_order(count)
    last, late = far[-1], near[2:]
    order = [("compute", 0), ("forward", far[0]), ("weights", 2), ("weights", 3)]
    order += [("send", k) for k in far[2:] + late]
    order += [("prepare", 0), ("forward", near[0]), ("pass_on", far[0])]
    order += [("compute", near[0]), ("compute", far[0])]
    order += [("forward", far[1]), ("forward", near[1]), ("forward", far[2]), ("compute", near[1])]
    order += [("gated", 0), ("gated", far[0]), ("down", 0), ("gated", near[0])]
    order += [("down", far[0]), ("pass_on", far[1]), ("down", near[0])]
    order += [("compute", far[1]), ("forward", last), ("gated", near[1])]
    order += [("pass_on", far[2]), ("down", near[1]), ("gated", far[1]), ("compute", far[2])]
    order += [("down", far[1])] + [("forward", k) for k in late] + [("pass_on", last)]
    order += [("compute", last), ("latents", 0), ("gated", far[2]), ("down", far[2])]
    order += [("gated", last)] + [("pass_on", k) for k in late] + [("down", last), ("give", last)]
    order += [("compute", k) for k in late] + [("relay", 0)]
    order += [("gated", k) for k in late]
    order += [("gather", 0)] + [("down", k) for k in late]
    order += [("attend", 0), ("settle", 0)]
    order += [("attend", head) for head in range(2, heads, 2)]
    return order


def dot_first(left, right):
    return lax.dot_general(
        left, right, (((0,), (0,)), ((), ())), preferred_element_type=jnp.float32
    )


def dot_f32(left, right):
    return jnp.dot(left, right, preferred_element_type=jnp.float32)


def window_kernel(
    count, capacity, base, ids_hbm, gates_hbm, latents_hbm, tokens_hbm, starts_hbm, gate_hbm, up_hbm,
    down_hbm, queries_hbm, uv_hbm, out_ref, attended_ref,
    ids, gates, latents, tokens, starts, pair_w, down_w, query_t, uv_w, every_latent, keys, value_t, seen, place, gate_of,
    outgoing, far_rows, extra_rows, arrived, hidden, back_send, collected, settled, returned, share, mixed,
    load_sem, lat_s, lat_r, out_s, out_r, side_s, side_r, near_s, near_r, relay_s, relay_r,
    hid_s, hid_r, wd_s, wd_r, back_s, back_r, fan_s, fan_r, collect_s, collect_r, settle_s, settle_r,
):
    me = lax.axis_index("exp")
    ctx = lax.axis_index("ctx")
    core = ctx % 2
    other_core = ctx + 1 - 2 * core
    other_row = (ctx + 2) % 4
    opposite = (other_core + 2) % 4
    peers = (other_core, other_row, opposite)
    width = outgoing.shape[3]
    token_count = tokens.shape[0]
    group = down_hbm.shape[1]
    part = group // down_parts
    fan = gate_hbm.shape[2]

    def columns(at):
        return pl.ds(pl.multiple_of(at * width, 128), width)

    inputs = [
        pltpu.make_async_copy(source, target, load_sem.at[5 + at])
        for at, (source, target) in enumerate(
            [(ids_hbm, ids), (tokens_hbm, tokens), (latents_hbm, latents), (gates_hbm, gates),
             (starts_hbm, starts)]
        )
    ]
    for load in inputs:
        load.start()
    loads = [
        pltpu.make_async_copy(gate_hbm.at[0], pair_w.at[:, pl.ds(0, fan)], load_sem.at[0]),
        pltpu.make_async_copy(up_hbm.at[0], pair_w.at[:, pl.ds(fan, fan)], load_sem.at[1]),
        pltpu.make_async_copy(queries_hbm, query_t, load_sem.at[3]),
        pltpu.make_async_copy(uv_hbm, uv_w, load_sem.at[4]),
        pltpu.make_async_copy(down_hbm.at[0, :, columns(ctx)], down_w.at[ctx], load_sem.at[2]),
    ]

    barrier = pltpu.get_barrier_semaphore()
    for k in range(1, count):
        pl.semaphore_signal(
            barrier, inc=1, device_id={"exp": flip_bits(me, k), "ctx": ctx},
            device_id_type=pl.DeviceIdType.MESH,
        )
    for peer in peers:
        pl.semaphore_signal(
            barrier, inc=1, device_id={"exp": me, "ctx": peer},
            device_id_type=pl.DeviceIdType.MESH,
        )

    def remote(source, target, send, recv, exp, ctx_at):
        return pltpu.make_async_remote_copy(
            src_ref=source, dst_ref=target, send_sem=send, recv_sem=recv,
            device_id={"exp": exp, "ctx": ctx_at}, device_id_type=pl.DeviceIdType.MESH,
        )

    half = count // 2
    rest = capacity - base
    far, near = list(range(half, count)), list(range(1, half))
    sequence = far_order(count)

    def far_start(k):
        return (k - half) * base + (rest if k > half else 0)

    def rows_of(k):
        return base if k > half else capacity

    def slots(k):
        if k < half:
            return pl.ds(k * capacity, capacity)
        return pl.ds(half * capacity + sequence.index(k) * base, base)

    extra_slots = pl.ds(half * (capacity + base), rest)
    low_rows, high_rows = pl.ds(0, base), pl.ds(base, rest)

    wide = near[:2]

    def copies_of(k):
        return 2 if k in wide else 1

    def dispatch(k):
        to = flip_bits(me, k)
        if k < half:
            pieces = [
                (outgoing.at[k, i], arrived.at[quarter, me])
                for i, quarter in enumerate((ctx, other_row)[: copies_of(k)])
            ]
        else:
            rows = rows_of(k)
            pieces = [
                (far_rows.at[pl.ds(far_start(k), rows)], arrived.at[ctx, me, pl.ds(0, rows)])
            ]
            if k == half:
                pieces += [(extra_rows, arrived.at[other_row, me, high_rows])]
        return [
            remote(source, target, out_s.at[k, i], out_r.at[k, i], to, ctx)
            for i, (source, target) in enumerate(pieces)
        ]

    def fan_out(k):
        blocks = [arrived.at[row, flip_bits(me, half), high_rows] for row in (ctx, other_row)]
        return [
            remote(block, block, fan_s.at[k, i], fan_r.at[k, i], flip_bits(me, k), ctx)
            for i, block in enumerate(blocks)
        ]

    def crossing(k, quarter):
        block = arrived.at[quarter, flip_bits(me, k)]
        return arrived.at[quarter, flip_bits(me, k), low_rows] if k >= half else block

    def across(k):
        block = crossing(k, ctx)
        return remote(block, block, side_s.at[k], side_r.at[k], me, other_row)

    def beside(k):
        at = flip_bits(me, k)
        blocks = [arrived.at[ctx, at]]
        if k >= half:
            blocks += [arrived.at[other_row, at, high_rows]]
        elif k in wide:
            blocks += [arrived.at[other_row, at]]
        return [
            remote(block, block, near_s.at[k, i], near_r.at[k, i], me, other_core)
            for i, block in enumerate(blocks)
        ]

    def relay(k):
        block = crossing(k, other_row)
        return remote(block, block, relay_s.at[k], relay_r.at[k], me, other_core)

    def share_hidden(k):
        block = hidden.at[k, ctx]
        return [
            remote(block, block, hid_s.at[k, i], hid_r.at[k, i], me, peer)
            for i, peer in enumerate((other_core, other_row))
        ]

    def relay_hidden(k):
        block = hidden.at[k, other_row]
        return remote(block, block, hid_s.at[k, 2], hid_r.at[k, 2], me, other_core)

    def share_down(i, piece):
        rows = pl.ds(piece * part, part)
        return remote(
            down_hbm.at[0, rows, columns(peers[i])], down_w.at[ctx, rows],
            wd_s.at[i, piece], wd_r.at[i, piece], me, peers[i],
        )

    def give_back(k):
        to = flip_bits(me, k)
        source = back_send.at[k, low_rows] if k >= half else back_send.at[k]
        return remote(source, returned.at[slots(k)], back_s.at[k], back_r.at[k], to, ctx)

    def collect(k):
        return remote(
            back_send.at[k + half, high_rows], collected.at[k], collect_s.at[k], collect_r.at[k],
            flip_bits(me, k), ctx,
        )

    def settle_extra():
        return remote(
            settled, returned.at[extra_slots], settle_s.at[0], settle_r.at[0],
            flip_bits(me, half), ctx,
        )

    def own_latents(step, peer):
        return remote(
            latents, every_latent.at[ctx], lat_s.at[step], lat_r.at[step], me, peer
        )

    row_block = every_latent.at[other_row]
    latents_beside = own_latents(0, other_core)
    latents_across = own_latents(1, other_row)
    latents_relay = remote(row_block, row_block, lat_s.at[2], lat_r.at[2], me, other_core)

    pl.semaphore_wait(barrier, count + 2)
    for piece in range(2):
        for i in (1, 2):
            share_down(i, piece).start()
    inputs[0].wait()
    inputs[3].wait()
    expert_at = lax.broadcasted_iota(jnp.int32, (count, token_count), 0)
    first, second = ids[0:1, :] == expert_at, ids[1:2, :] == expert_at
    member = first | second
    before = lax.broadcasted_iota(jnp.int32, (token_count, token_count), 0)
    after = lax.broadcasted_iota(jnp.int32, (token_count, token_count), 1)
    earlier = dot_f32(
        member.astype(jnp.float32).astype(jnp.bfloat16),
        (before < after).astype(jnp.float32).astype(jnp.bfloat16),
    )
    place[...] = jnp.where(member, earlier, -1.0)
    gate_of[...] = jnp.where(first, gates[0:1, :], 0.0) + jnp.where(second, gates[1:2, :], 0.0)
    slot_at = lax.broadcasted_iota(jnp.int32, (capacity, token_count), 0).astype(jnp.float32)

    def row_of(ref, k):
        return ref[pl.ds(flip_bits(me, k), 1), :]

    def one_hot(k, first_slot, last_slot):
        return (row_of(place, k) == slot_at[first_slot:last_slot]).astype(jnp.float32)

    def take(picks, column):
        rows = dot_f32(picks.astype(jnp.bfloat16), tokens[:, columns(column)])
        return rows.astype(jnp.bfloat16)

    def select(ks, i, column):
        rows = take(jnp.concatenate([one_hot(k, 0, capacity) for k in ks], axis=0), column)
        for at, k in enumerate(ks):
            outgoing[k, i] = rows[at * capacity : (at + 1) * capacity]

    def select_far():
        picks = [one_hot(k, 0, base) for k in far]
        extra = one_hot(half, base, capacity)
        for k in far[1:]:
            extra += one_hot(k, base, capacity)
        far_rows[...] = take(jnp.concatenate(picks[:1] + [extra] + picks[1:], axis=0), ctx)
        extra_rows[...] = take(extra, other_row)

    def send(k):
        for copy in dispatch(k):
            copy.start()

    inputs[1].wait()
    select_far()
    send(sequence[0])
    select(near, 0, ctx)
    select(wide, 1, other_row)
    send(near[1])
    send(near[0])
    send(sequence[1])
    for load in loads:
        load.start()
    for piece in range(down_parts):
        share_down(0, piece).start()
    inputs[2].wait()
    latents_beside.start()
    every_latent[ctx] = latents[...]
    mine = one_hot(0, 0, capacity).astype(jnp.bfloat16)
    for quarter in range(4):
        span = pl.ds(quarter * width, width)
        arrived[quarter, me] = dot_f32(mine, tokens[:, span]).astype(jnp.bfloat16)

    span_tokens = latents.shape[1]
    half_block = span_tokens // 2
    lat_width = uv_w.shape[1]

    def send_latents(_):
        latents_across.start()

    def relay_latents(_):
        latents_across.wait_recv()
        latents_relay.start()

    def gather_latents(_):
        inputs[4].wait()
        key_at = lax.broadcasted_iota(jnp.int32, (4 * span_tokens, span_tokens), 0)
        own_at = lax.broadcasted_iota(jnp.int32, (4 * span_tokens, span_tokens), 1)
        key_block = key_at // half_block
        key_start = jnp.zeros_like(key_at)
        for block in range(8):
            key_start = jnp.where(key_block == block, starts[block], key_start)
        own_start = jnp.where(own_at < half_block, starts[2 * ctx], starts[2 * ctx + 1])
        key_position = key_start + key_at % half_block
        seen[...] = (key_position <= own_start + own_at % half_block).astype(jnp.float32)
        latents_beside.wait_recv()
        latents_relay.wait_recv()
        for block in range(4):
            span = pl.ds(block * span_tokens, span_tokens)
            value_t[:, span] = every_latent[block, :lat_width, :]
            keys[span, :] = every_latent[block].T
        for load in loads[2:4]:
            load.wait()

    def attend(head):
        pair = range(head, min(head + 2, query_t.shape[0]))
        wide_query = jnp.concatenate([query_t[at] for at in pair], axis=1)
        visible = jnp.concatenate([seen[...] for _ in pair], axis=1) > 0.5
        scores = dot_f32(keys[...], wide_query) * score_scale
        masked = jnp.where(visible, scores, neg_fill)
        top = jnp.max(masked, axis=0, keepdims=True)
        weights = jnp.where(visible, jnp.exp(masked - top), 0.0)
        totals = jnp.sum(weights, axis=0, keepdims=True)
        blended = dot_f32(value_t[...], weights.astype(jnp.bfloat16))
        latent_out = (blended / totals).astype(jnp.bfloat16)
        for spot, at in enumerate(pair):
            span = slice(spot * span_tokens, (spot + 1) * span_tokens)
            attended_ref[at] = dot_first(latent_out[:, span], uv_w[at]).astype(jnp.bfloat16)

    def forward(k):
        for copy in dispatch(k):
            copy.wait_recv()
        if k == half:
            for other in sequence[1:]:
                for copy in fan_out(other - half):
                    copy.start()
        elif k > half:
            for copy in fan_out(k - half):
                copy.wait_recv()
        if k not in wide:
            across(k).start()
        for copy in beside(k):
            copy.start()

    def weights(piece):
        for i in (1, 2):
            share_down(i, piece).start()

    def pass_on(k):
        across(k).wait_recv()
        relay(k).start()

    def compute(k):
        if k:
            for copy in beside(k):
                copy.wait_recv()
            if k not in wide:
                relay(k).wait_recv()
        else:
            loads[0].wait()
            loads[1].wait()
        at = flip_bits(me, k)
        both = jnp.zeros((capacity, 2 * fan), jnp.float32)
        for quarter in range(4):
            both += dot_f32(arrived[quarter, at], pair_w[pl.ds(quarter * width, width), :])
        gate_h, up_h = both[:, :fan], both[:, fan:]
        hidden[k, ctx] = (gate_h / (1.0 + jnp.exp(-gate_h)) * up_h).astype(jnp.bfloat16)
        for copy in share_hidden(k):
            copy.start()

    waiting = [loads[4]]
    is_full = jnp.max(row_of(place, 0), axis=1, keepdims=True) >= float(base)

    def down(k):
        while waiting:
            waiting.pop().wait()
            for i in range(3):
                for piece in range(down_parts):
                    share_down(i, piece).wait_recv()
        share_hidden(k)[0].wait_recv()
        relay_hidden(k).wait_recv()
        total = dot_f32(hidden[k, 0], down_w[0])
        for block in range(1, 4):
            total += dot_f32(hidden[k, block], down_w[block])
        if k == 0:
            returned[slots(0)] = total.astype(jnp.bfloat16)
            return
        if k >= half:
            back_send[k, low_rows] = total[:base].astype(jnp.bfloat16)
            back_send[k, high_rows] = jnp.where(is_full, total[base:], 0.0).astype(jnp.bfloat16)
        else:
            back_send[k] = total.astype(jnp.bfloat16)
        if k > half:
            collect(k - half).start()
        if k != sequence[-1]:
            give_back(k).start()

    def give(k):
        give_back(k).start()

    def gated(k):
        share_hidden(k)[1].wait_recv()
        relay_hidden(k).start()

    def settle(_):
        extra = back_send[half, high_rows].astype(jnp.float32)
        for k in near:
            collect(k).wait_recv()
            extra += collected[k].astype(jnp.float32)
        settled[...] = extra.astype(jnp.bfloat16)
        settle_extra().start()

    early = half * capacity + (half - 2) * base
    total_rows = half * (capacity + base) + rest

    def prepare(_):
        def share_of(k, first_slot, last_slot):
            return one_hot(k, first_slot, last_slot) * row_of(gate_of, k)

        extra = share_of(half, base, capacity)
        for k in far[1:]:
            extra += share_of(k, base, capacity)
        spread = jnp.concatenate(
            [share_of(k, 0, capacity) for k in range(half)]
            + [share_of(k, 0, base) for k in sequence]
            + [extra],
            axis=0,
        )
        pad = jnp.zeros((share.shape[2] - total_rows, token_count), jnp.float32)
        spread = jnp.concatenate([spread, pad], axis=0).T
        high = spread.astype(jnp.bfloat16)
        share[0] = high
        share[1] = (spread - high.astype(jnp.float32)).astype(jnp.bfloat16)

    def mix(first_row, last_row):
        rows = returned[first_row:last_row]
        high, low = share[0, :, first_row:last_row], share[1, :, first_row:last_row]
        return dot_f32(high, rows) + dot_f32(low, rows)

    stages = {
        "forward": forward, "pass_on": pass_on, "compute": compute, "down": down,
        "attend": attend, "latents": send_latents, "gather": gather_latents, "relay": relay_latents, "give": give, "weights": weights,
        "settle": settle, "prepare": prepare, "send": send, "gated": gated,
    }
    for stage, at in plan(count, query_t.shape[0]):
        stages[stage](at)

    for k in near + sequence[: half - 2]:
        give_back(k).wait_recv()
    mixed[...] = mix(0, early)
    for k in sequence[half - 2 :]:
        give_back(k).wait_recv()
    settle_extra().wait_recv()
    out_ref[...] = (mixed[...] + mix(early, total_rows)).astype(jnp.bfloat16)
    for copy in (latents_across, latents_beside, latents_relay, settle_extra()):
        copy.wait_send()
    for i in range(3):
        for piece in range(down_parts):
            share_down(i, piece).wait_send()
    for k in range(count):
        copies = share_hidden(k) + [relay_hidden(k)]
        if k:
            copies += dispatch(k) + beside(k) + [give_back(k)]
            if k < half:
                copies += fan_out(k) + [collect(k)]
            if k not in wide:
                copies += [across(k), relay(k)]
        for copy in copies:
            copy.wait_send()


def base_rows(row_count, capacity, count):
    spare = -(-(row_count - capacity) // (count - 1))
    return 16 * -(-spare // 16)


def window_fused(
    queries, latents, block_starts, w_uv, moe_tokens, expert_ids, gate_weights, w_gate, w_up, w_down
):
    queries = jnp.transpose(queries, (1, 2, 0))
    heads, entry_width, query_tokens = queries.shape
    lat_width, value_width = w_uv.shape[1:]
    ways = lax.axis_size("ctx")
    key_count = ways * query_tokens
    token_count, picks = expert_ids.shape
    model_width = moe_tokens.shape[1]
    fan = w_gate.shape[2]
    count = lax.axis_size("exp")
    width = model_width // ways
    capacity = 3 * token_count * picks // (2 * count)
    half = count // 2
    base = base_rows(token_count * picks, capacity, count)
    rest = capacity - base
    share_width = 128 * -(-(half * (capacity + base) + rest) // 128)
    vmem = pl.BlockSpec(memory_space=pltpu.VMEM)
    hbm = pl.BlockSpec(memory_space=pltpu.HBM)
    block = (capacity, width)
    dtype = jnp.bfloat16
    dma = pltpu.SemaphoreType.DMA
    routed, attended = pl.pallas_call(
        functools.partial(window_kernel, count, capacity, base),
        out_shape=(
            jax.ShapeDtypeStruct((token_count, width), dtype),
            jax.ShapeDtypeStruct((heads, query_tokens, value_width), dtype),
        ),
        in_specs=[hbm] * 10,
        out_specs=(vmem, vmem),
        scratch_shapes=[
            pltpu.VMEM((picks, token_count), jnp.int32),
            pltpu.VMEM((picks, token_count), jnp.float32),
            pltpu.VMEM((entry_width, query_tokens), dtype),
            pltpu.VMEM((token_count, model_width), dtype),
            pltpu.SMEM(block_starts.shape, jnp.int32),
            pltpu.VMEM((model_width, 2 * fan), dtype),
            pltpu.VMEM((ways, fan, width), dtype),
            pltpu.VMEM(queries.shape, dtype),
            pltpu.VMEM(w_uv.shape, dtype),
            pltpu.VMEM((ways, entry_width, query_tokens), dtype),
            pltpu.VMEM((key_count, entry_width), dtype),
            pltpu.VMEM((lat_width, key_count), dtype),
            pltpu.VMEM((key_count, query_tokens), jnp.float32),
            pltpu.VMEM((count, token_count), jnp.float32),
            pltpu.VMEM((count, token_count), jnp.float32),
            pltpu.VMEM((half, 2) + block, dtype),
            pltpu.VMEM((half * base + rest, width), dtype),
            pltpu.VMEM((rest, width), dtype),
            pltpu.VMEM((ways, count) + block, dtype),
            pltpu.VMEM((count, ways, capacity, fan), dtype),
            pltpu.VMEM((count,) + block, dtype),
            pltpu.VMEM((half, rest, width), dtype),
            pltpu.VMEM((rest, width), dtype),
            pltpu.VMEM((half * (capacity + base) + rest, width), dtype),
            pltpu.VMEM((2, token_count, share_width), dtype),
            pltpu.VMEM((token_count, width), jnp.float32),
            dma((10,)), dma((3,)), dma((3,)),
            dma((count, 2)), dma((count, 2)),
            dma((count,)), dma((count,)),
            dma((count, 2)), dma((count, 2)),
            dma((count,)), dma((count,)),
            dma((count, 3)), dma((count, 3)),
            dma((3, down_parts)), dma((3, down_parts)),
            dma((count,)), dma((count,)),
            dma((half, 2)), dma((half, 2)),
            dma((half,)), dma((half,)),
            dma((1,)), dma((1,)),
        ],
        compiler_params=pltpu.CompilerParams(
            collective_id=0, has_side_effects=True, vmem_limit_bytes=40 * 1024 * 1024
        ),
    )(
        *[
            pltpu.with_memory_space_constraint(operand, pltpu.HBM)
            for operand in (
                expert_ids.T, gate_weights.T, latents.T, moe_tokens, block_starts,
                w_gate, w_up, w_down, queries, w_uv,
            )
        ]
    )
    return jnp.transpose(attended, (1, 0, 2)), routed


def shards(
    queries, latents, block_starts, w_uv, moe_tokens, expert_ids, gate_weights, w_gate, w_up, w_down
):
    count = lax.axis_size("exp")
    ways = lax.axis_size("ctx")
    token_count, picks = expert_ids.shape
    capacity = 3 * token_count * picks // (2 * count)
    fits = ways == 4 and count & (count - 1) == 0 and count >= 4 and capacity % 16 == 0
    fits = fits and moe_tokens.shape[1] % (128 * ways) == 0 and block_starts.shape[0] == 8
    base = base_rows(token_count * picks, capacity, count)
    fits = fits and base < capacity and count >= 8
    fits = fits and picks == 2 and w_gate.shape[2] % 128 == 0
    if fits:
        return window_fused(
            queries, latents, block_starts, w_uv, moe_tokens, expert_ids, gate_weights,
            w_gate, w_up, w_down,
        )
    attended = attention(queries, latents, block_starts, w_uv)
    return attended, routed_plain(moe_tokens, expert_ids, gate_weights, w_gate, w_up, w_down)


def solution(mesh):
    in_specs = (
        P("ctx", "exp", None),
        P("ctx", None),
        P(),
        P("exp", None, None),
        P("exp", None),
        P("exp", None),
        P("exp", None),
        P("exp", None, "ctx"),
        P("exp", None, "ctx"),
        P("exp", "ctx", None),
    )
    out_specs = (P("ctx", "exp", None), P("exp", "ctx"))
    return jax.shard_map(shards, mesh=mesh, in_specs=in_specs, out_specs=out_specs, check_vma=False)
```

```python
import functools
import math

import jax
import jax.numpy as jnp
from jax import lax
from jax.experimental import pallas as pl
from jax.experimental.pallas import tpu as pltpu
from jax.sharding import PartitionSpec as P

score_scale = (0.1 * math.log(40.0) + 1.0) ** 2 / math.sqrt(192.0)
neg_fill = -1e30


def token_positions(block_starts, token_index, half_block):
    block_index = token_index // half_block
    matches = block_index[:, None] == jnp.arange(block_starts.shape[0], dtype=jnp.int32)[None, :]
    first_pos = jnp.sum(jnp.where(matches, block_starts[None, :], 0), axis=1)
    return first_pos + token_index % half_block


def slot_targets(expert_ids, expert_count, capacity):
    token_count, picks = expert_ids.shape
    flat_ids = expert_ids.reshape(token_count * picks)
    onehot = (flat_ids[:, None] == jnp.arange(expert_count, dtype=jnp.int32)[None, :]).astype(
        jnp.int32
    )
    earlier = jnp.cumsum(onehot, axis=0) - onehot
    slot_index = jnp.sum(earlier * onehot, axis=1)
    return flat_ids * capacity + slot_index


def attention(queries, latents, block_starts, w_uv):
    query_tokens, head_count, entry_width = queries.shape
    lat_width = w_uv.shape[1]
    half_block = query_tokens // 2
    row_total = query_tokens * head_count
    flat_queries = queries.reshape(row_total, entry_width)
    own_index = lax.axis_index("ctx") * query_tokens + jnp.arange(query_tokens, dtype=jnp.int32)
    own_positions = token_positions(block_starts, own_index, half_block)
    query_positions = jnp.repeat(own_positions, head_count)
    shard_piece = lax.all_gather(latents, "ctx", axis=0, tiled=True)
    key_positions = token_positions(
        block_starts, jnp.arange(shard_piece.shape[0], dtype=jnp.int32), half_block
    )
    top_score = jnp.full((row_total,), neg_fill, jnp.float32)
    scores = (
        lax.dot_general(
            flat_queries, shard_piece, (((1,), (1,)), ((), ())), preferred_element_type=jnp.float32
        )
        * score_scale
    )
    visible = key_positions[None, :] <= query_positions[:, None]
    masked = jnp.where(visible, scores, neg_fill)
    new_top = jnp.maximum(top_score, jnp.max(masked, axis=1))
    weights = jnp.where(visible, jnp.exp(masked - new_top[:, None]), 0.0)
    totals = jnp.sum(weights, axis=1)
    blended = jnp.dot(
        weights.astype(jnp.bfloat16), shard_piece[:, :lat_width], preferred_element_type=jnp.float32
    )
    top_score, totals, blended = (new_top, totals, blended)
    latent_out = (
        (blended / totals[:, None])
        .astype(jnp.bfloat16)
        .reshape(query_tokens, head_count, lat_width)
    )
    attended = jnp.einsum(
        "shl,hlv->shv", latent_out, w_uv, preferred_element_type=jnp.float32
    ).astype(jnp.bfloat16)
    return attended


def routed_plain(moe_tokens, expert_ids, gate_weights, w_gate, w_up, w_down):
    token_count, picks = expert_ids.shape
    model_width = moe_tokens.shape[1]
    expert_count = lax.axis_size("exp")
    capacity = 3 * token_count * picks // (2 * expert_count)
    targets = slot_targets(expert_ids, expert_count, capacity)
    source_row = jnp.arange(token_count * picks, dtype=jnp.int32) // picks
    filled = jnp.zeros((expert_count * capacity,), jnp.int32).at[targets].set(source_row + 1)
    occupied = filled > 0
    gate_matrix = w_gate[0]
    up_matrix = w_up[0]
    down_matrix = w_down[0]
    picked_rows = moe_tokens[jnp.where(occupied, filled - 1, 0)]
    outgoing = jnp.where(occupied[:, None], picked_rows, 0).reshape(
        expert_count, capacity, model_width
    )
    arrived = lax.all_to_all(outgoing, "exp", split_axis=0, concat_axis=0, tiled=True)
    senders, slot_count, width_in = arrived.shape
    flat_rows = arrived.reshape(senders * slot_count, width_in)
    gate_h = jnp.dot(flat_rows, gate_matrix, preferred_element_type=jnp.float32)
    up_h = jnp.dot(flat_rows, up_matrix, preferred_element_type=jnp.float32)
    hidden = (jax.nn.silu(gate_h) * up_h).astype(jnp.bfloat16)
    rounded = jnp.dot(hidden, down_matrix, preferred_element_type=jnp.float32).astype(jnp.bfloat16)
    rounded = lax.optimization_barrier(rounded.reshape(senders, slot_count, width_in))
    summed = lax.psum_scatter(
        rounded.astype(jnp.float32).astype(jnp.bfloat16), "ctx", scatter_dimension=2, tiled=True
    ).astype(jnp.float32)
    returned = lax.all_to_all(
        summed.astype(jnp.bfloat16), "exp", split_axis=0, concat_axis=0, tiled=True
    ).astype(summed.dtype)
    out_width = returned.shape[2]
    gathered = returned.reshape(expert_count * capacity, out_width)[targets].reshape(
        token_count, picks, out_width
    )
    weighted = jnp.sum(gathered * gate_weights[:, :, None], axis=1)
    return weighted.astype(jnp.bfloat16)


def flip_bits(index, bits):
    flipped = index
    for bit in range(bits.bit_length()):
        if (bits >> bit) % 2:
            flipped = flipped + (1 << bit) * (1 - 2 * ((index // (1 << bit)) % 2))
    return flipped


down_parts = 4


def far_order(count):
    half = count // 2
    return [half, half + 1] + list(range(count - 1, half + 1, -1))


def plan(count, heads):
    half = count // 2
    near, far = list(range(1, half)), far_order(count)
    last, late = far[-1], near[2:]
    order = [("compute", 0), ("forward", far[0]), ("weights", 2), ("weights", 3)]
    order += [("send", k) for k in far[2:] + late]
    order += [("prepare", 0), ("forward", near[0]), ("pass_on", far[0])]
    order += [("compute", near[0]), ("compute", far[0])]
    order += [("forward", far[1]), ("forward", near[1]), ("forward", far[2]), ("compute", near[1])]
    order += [("gated", 0), ("gated", far[0]), ("down", 0), ("gated", near[0])]
    order += [("down", far[0]), ("pass_on", far[1]), ("down", near[0])]
    order += [("compute", far[1]), ("forward", last), ("gated", near[1])]
    order += [("pass_on", far[2]), ("down", near[1]), ("gated", far[1]), ("compute", far[2])]
    order += [("down", far[1])] + [("forward", k) for k in late] + [("pass_on", last)]
    order += [("compute", last), ("latents", 0), ("gated", far[2]), ("down", far[2])]
    order += [("gated", last)] + [("pass_on", k) for k in late] + [("down", last), ("give", last)]
    order += [("compute", k) for k in late] + [("relay", 0)]
    order += [("gated", k) for k in late]
    order += [("gather", 0)] + [("down", k) for k in late]
    order += [("attend", 0), ("settle", 0)]
    order += [("attend", head) for head in range(2, heads, 2)]
    return order


def dot_first(left, right):
    return lax.dot_general(
        left, right, (((0,), (0,)), ((), ())), preferred_element_type=jnp.float32
    )


def dot_f32(left, right):
    return jnp.dot(left, right, preferred_element_type=jnp.float32)


def window_kernel(
    count, capacity, base, ids_hbm, gates_hbm, latents_hbm, tokens_hbm, starts_hbm, gate_hbm, up_hbm,
    down_hbm, queries_hbm, uv_hbm, out_ref, attended_ref,
    ids, gates, latents, tokens, starts, pair_w, down_w, query_t, uv_w, every_latent, keys, value_t, seen, place, gate_of,
    outgoing, far_rows, extra_rows, arrived, hidden, back_send, collected, settled, returned, share, mixed,
    load_sem, lat_s, lat_r, sent, out_r, side_r, near_r, relay_r,
    hid_r, wd_r, back_r, fan_r, collect_r, settle_r,
):
    me = lax.axis_index("exp")
    ctx = lax.axis_index("ctx")
    core = ctx % 2
    other_core = ctx + 1 - 2 * core
    other_row = (ctx + 2) % 4
    opposite = (other_core + 2) % 4
    peers = (other_core, other_row, opposite)
    width = outgoing.shape[3]
    token_count = tokens.shape[0]
    group = down_hbm.shape[1]
    part = group // down_parts
    fan = gate_hbm.shape[2]

    def columns(at):
        return pl.ds(pl.multiple_of(at * width, 128), width)

    inputs = [
        pltpu.make_async_copy(source, target, load_sem.at[5 + at])
        for at, (source, target) in enumerate(
            [(ids_hbm, ids), (tokens_hbm, tokens), (latents_hbm, latents), (gates_hbm, gates),
             (starts_hbm, starts)]
        )
    ]
    for load in inputs:
        load.start()
    loads = [
        pltpu.make_async_copy(gate_hbm.at[0], pair_w.at[:, pl.ds(0, fan)], load_sem.at[0]),
        pltpu.make_async_copy(up_hbm.at[0], pair_w.at[:, pl.ds(fan, fan)], load_sem.at[1]),
        pltpu.make_async_copy(queries_hbm, query_t, load_sem.at[3]),
        pltpu.make_async_copy(uv_hbm, uv_w, load_sem.at[4]),
        pltpu.make_async_copy(down_hbm.at[0, :, columns(ctx)], down_w.at[ctx], load_sem.at[2]),
    ]

    barrier = pltpu.get_barrier_semaphore()
    for k in range(1, count):
        pl.semaphore_signal(
            barrier, inc=1, device_id={"exp": flip_bits(me, k), "ctx": ctx},
            device_id_type=pl.DeviceIdType.MESH,
        )
    for peer in peers:
        pl.semaphore_signal(
            barrier, inc=1, device_id={"exp": me, "ctx": peer},
            device_id_type=pl.DeviceIdType.MESH,
        )

    def remote(source, target, send, recv, exp, ctx_at):
        return pltpu.make_async_remote_copy(
            src_ref=source, dst_ref=target, send_sem=send, recv_sem=recv,
            device_id={"exp": exp, "ctx": ctx_at}, device_id_type=pl.DeviceIdType.MESH,
        )

    half = count // 2
    rest = capacity - base
    far, near = list(range(half, count)), list(range(1, half))
    sequence = far_order(count)

    def far_start(k):
        return (k - half) * base + (rest if k > half else 0)

    def rows_of(k):
        return base if k > half else capacity

    def slots(k):
        if k < half:
            return pl.ds(k * capacity, capacity)
        return pl.ds(half * capacity + sequence.index(k) * base, base)

    extra_slots = pl.ds(half * (capacity + base), rest)
    low_rows, high_rows = pl.ds(0, base), pl.ds(base, rest)

    wide = near[:2]

    def copies_of(k):
        return 2 if k in wide else 1

    def dispatch(k):
        to = flip_bits(me, k)
        if k < half:
            pieces = [
                (outgoing.at[k, i], arrived.at[quarter, me])
                for i, quarter in enumerate((ctx, other_row)[: copies_of(k)])
            ]
        else:
            rows = rows_of(k)
            pieces = [
                (far_rows.at[pl.ds(far_start(k), rows)], arrived.at[ctx, me, pl.ds(0, rows)])
            ]
            if k == half:
                pieces += [(extra_rows, arrived.at[other_row, me, high_rows])]
        return [
            remote(source, target, sent.at[0], out_r.at[k, i], to, ctx)
            for i, (source, target) in enumerate(pieces)
        ]

    def fan_out(k):
        blocks = [arrived.at[row, flip_bits(me, half), high_rows] for row in (ctx, other_row)]
        return [
            remote(block, block, sent.at[0], fan_r.at[k, i], flip_bits(me, k), ctx)
            for i, block in enumerate(blocks)
        ]

    def crossing(k, quarter):
        block = arrived.at[quarter, flip_bits(me, k)]
        return arrived.at[quarter, flip_bits(me, k), low_rows] if k >= half else block

    def across(k):
        block = crossing(k, ctx)
        return remote(block, block, sent.at[0], side_r.at[k], me, other_row)

    def beside(k):
        at = flip_bits(me, k)
        blocks = [arrived.at[ctx, at]]
        if k >= half:
            blocks += [arrived.at[other_row, at, high_rows]]
        elif k in wide:
            blocks += [arrived.at[other_row, at]]
        return [
            remote(block, block, sent.at[0], near_r.at[k, i], me, other_core)
            for i, block in enumerate(blocks)
        ]

    def relay(k):
        block = crossing(k, other_row)
        return remote(block, block, sent.at[0], relay_r.at[k], me, other_core)

    def share_hidden(k):
        block = hidden.at[k, ctx]
        return [
            remote(block, block, sent.at[2], hid_r.at[k, i], me, peer)
            for i, peer in enumerate((other_core, other_row))
        ]

    def relay_hidden(k):
        block = hidden.at[k, other_row]
        return remote(block, block, sent.at[2], hid_r.at[k, 2], me, other_core)

    def share_down(i, piece):
        rows = pl.ds(piece * part, part)
        return remote(
            down_hbm.at[0, rows, columns(peers[i])], down_w.at[ctx, rows],
            sent.at[3], wd_r.at[0], me, peers[i],
        )

    def give_back(k):
        to = flip_bits(me, k)
        source = back_send.at[k, low_rows] if k >= half else back_send.at[k]
        return remote(source, returned.at[slots(k)], sent.at[0 if k >= half else 1], back_r.at[k], to, ctx)

    def collect(k):
        return remote(
            back_send.at[k + half, high_rows], collected.at[k], sent.at[0], collect_r.at[k],
            flip_bits(me, k), ctx,
        )

    def settle_extra():
        return remote(
            settled, returned.at[extra_slots], sent.at[0], settle_r.at[0],
            flip_bits(me, half), ctx,
        )

    def own_latents(step, peer):
        return remote(
            latents, every_latent.at[ctx], lat_s.at[step], lat_r.at[step], me, peer
        )

    row_block = every_latent.at[other_row]
    latents_beside = own_latents(0, other_core)
    latents_across = own_latents(1, other_row)
    latents_relay = remote(row_block, row_block, lat_s.at[2], lat_r.at[2], me, other_core)

    pl.semaphore_wait(barrier, count + 2)
    for piece in range(2):
        for i in (1, 2):
            share_down(i, piece).start()
    inputs[0].wait()
    inputs[3].wait()
    expert_at = lax.broadcasted_iota(jnp.int32, (count, token_count), 0)
    first, second = ids[0:1, :] == expert_at, ids[1:2, :] == expert_at
    member = first | second
    before = lax.broadcasted_iota(jnp.int32, (token_count, token_count), 0)
    after = lax.broadcasted_iota(jnp.int32, (token_count, token_count), 1)
    earlier = dot_f32(
        member.astype(jnp.float32).astype(jnp.bfloat16),
        (before < after).astype(jnp.float32).astype(jnp.bfloat16),
    )
    place[...] = jnp.where(member, earlier, -1.0)
    gate_of[...] = jnp.where(first, gates[0:1, :], 0.0) + jnp.where(second, gates[1:2, :], 0.0)
    slot_at = lax.broadcasted_iota(jnp.int32, (capacity, token_count), 0).astype(jnp.float32)

    def row_of(ref, k):
        return ref[pl.ds(flip_bits(me, k), 1), :]

    def one_hot(k, first_slot, last_slot):
        return (row_of(place, k) == slot_at[first_slot:last_slot]).astype(jnp.float32)

    def take(picks, column):
        rows = dot_f32(picks.astype(jnp.bfloat16), tokens[:, columns(column)])
        return rows.astype(jnp.bfloat16)

    def select(ks, i, column):
        rows = take(jnp.concatenate([one_hot(k, 0, capacity) for k in ks], axis=0), column)
        for at, k in enumerate(ks):
            outgoing[k, i] = rows[at * capacity : (at + 1) * capacity]

    def select_far():
        picks = [one_hot(k, 0, base) for k in far]
        extra = one_hot(half, base, capacity)
        for k in far[1:]:
            extra += one_hot(k, base, capacity)
        far_rows[...] = take(jnp.concatenate(picks[:1] + [extra] + picks[1:], axis=0), ctx)
        extra_rows[...] = take(extra, other_row)

    def send(k):
        for copy in dispatch(k):
            copy.start()

    inputs[1].wait()
    select_far()
    send(sequence[0])
    select(near, 0, ctx)
    select(wide, 1, other_row)
    send(near[1])
    send(near[0])
    send(sequence[1])
    for load in loads:
        load.start()
    for piece in range(down_parts):
        share_down(0, piece).start()
    inputs[2].wait()
    latents_beside.start()
    every_latent[ctx] = latents[...]
    mine = one_hot(0, 0, capacity).astype(jnp.bfloat16)
    for quarter in range(4):
        span = pl.ds(quarter * width, width)
        arrived[quarter, me] = dot_f32(mine, tokens[:, span]).astype(jnp.bfloat16)

    span_tokens = latents.shape[1]
    half_block = span_tokens // 2
    lat_width = uv_w.shape[1]

    def send_latents(_):
        latents_across.start()

    def relay_latents(_):
        latents_across.wait_recv()
        latents_relay.start()

    def gather_latents(_):
        inputs[4].wait()
        key_at = lax.broadcasted_iota(jnp.int32, (4 * span_tokens, span_tokens), 0)
        own_at = lax.broadcasted_iota(jnp.int32, (4 * span_tokens, span_tokens), 1)
        key_block = key_at // half_block
        key_start = jnp.zeros_like(key_at)
        for block in range(8):
            key_start = jnp.where(key_block == block, starts[block], key_start)
        own_start = jnp.where(own_at < half_block, starts[2 * ctx], starts[2 * ctx + 1])
        key_position = key_start + key_at % half_block
        seen[...] = (key_position <= own_start + own_at % half_block).astype(jnp.float32)
        latents_beside.wait_recv()
        latents_relay.wait_recv()
        for block in range(4):
            span = pl.ds(block * span_tokens, span_tokens)
            value_t[:, span] = every_latent[block, :lat_width, :]
            keys[span, :] = every_latent[block].T
        for load in loads[2:4]:
            load.wait()

    def attend(head):
        pair = range(head, min(head + 2, query_t.shape[0]))
        wide_query = jnp.concatenate([query_t[at] for at in pair], axis=1)
        visible = jnp.concatenate([seen[...] for _ in pair], axis=1) > 0.5
        scores = dot_f32(keys[...], wide_query) * score_scale
        masked = jnp.where(visible, scores, neg_fill)
        top = jnp.max(masked, axis=0, keepdims=True)
        weights = jnp.where(visible, jnp.exp(masked - top), 0.0)
        totals = jnp.sum(weights, axis=0, keepdims=True)
        blended = dot_f32(value_t[...], weights.astype(jnp.bfloat16))
        latent_out = (blended / totals).astype(jnp.bfloat16)
        for spot, at in enumerate(pair):
            span = slice(spot * span_tokens, (spot + 1) * span_tokens)
            attended_ref[at] = dot_first(latent_out[:, span], uv_w[at]).astype(jnp.bfloat16)

    def forward(k):
        for copy in dispatch(k):
            copy.wait_recv()
        if k == half:
            for other in sequence[1:]:
                for copy in fan_out(other - half):
                    copy.start()
        elif k > half:
            for copy in fan_out(k - half):
                copy.wait_recv()
        if k not in wide:
            across(k).start()
        for copy in beside(k):
            copy.start()

    def weights(piece):
        for i in (1, 2):
            share_down(i, piece).start()

    def pass_on(k):
        across(k).wait_recv()
        relay(k).start()

    def compute(k):
        if k:
            for copy in beside(k):
                copy.wait_recv()
            if k not in wide:
                relay(k).wait_recv()
        else:
            loads[0].wait()
            loads[1].wait()
        at = flip_bits(me, k)
        both = jnp.zeros((capacity, 2 * fan), jnp.float32)
        for quarter in range(4):
            both += dot_f32(arrived[quarter, at], pair_w[pl.ds(quarter * width, width), :])
        gate_h, up_h = both[:, :fan], both[:, fan:]
        hidden[k, ctx] = (gate_h / (1.0 + jnp.exp(-gate_h)) * up_h).astype(jnp.bfloat16)
        for copy in share_hidden(k):
            copy.start()

    waiting = [loads[4]]
    three = down_w.at[pl.ds(0, 3)]
    all_down = remote(three, three, sent.at[3], wd_r.at[0], me, other_core)
    is_full = jnp.max(row_of(place, 0), axis=1, keepdims=True) >= float(base)

    def down(k):
        while waiting:
            waiting.pop().wait()
            all_down.wait_recv()
        share_hidden(k)[0].wait_recv()
        relay_hidden(k).wait_recv()
        total = dot_f32(hidden[k, 0], down_w[0])
        for block in range(1, 4):
            total += dot_f32(hidden[k, block], down_w[block])
        if k == 0:
            returned[slots(0)] = total.astype(jnp.bfloat16)
            return
        if k >= half:
            back_send[k, low_rows] = total[:base].astype(jnp.bfloat16)
            back_send[k, high_rows] = jnp.where(is_full, total[base:], 0.0).astype(jnp.bfloat16)
        else:
            back_send[k] = total.astype(jnp.bfloat16)
        if k > half:
            collect(k - half).start()
        if k != sequence[-1]:
            give_back(k).start()

    def give(k):
        give_back(k).start()

    def gated(k):
        share_hidden(k)[1].wait_recv()
        relay_hidden(k).start()

    def settle(_):
        extra = back_send[half, high_rows].astype(jnp.float32)
        for k in near:
            collect(k).wait_recv()
            extra += collected[k].astype(jnp.float32)
        settled[...] = extra.astype(jnp.bfloat16)
        settle_extra().start()

    early = half * capacity + (half - 2) * base
    total_rows = half * (capacity + base) + rest

    def prepare(_):
        def share_of(k, first_slot, last_slot):
            return one_hot(k, first_slot, last_slot) * row_of(gate_of, k)

        extra = share_of(half, base, capacity)
        for k in far[1:]:
            extra += share_of(k, base, capacity)
        spread = jnp.concatenate(
            [share_of(k, 0, capacity) for k in range(half)]
            + [share_of(k, 0, base) for k in sequence]
            + [extra],
            axis=0,
        )
        pad = jnp.zeros((share.shape[2] - total_rows, token_count), jnp.float32)
        spread = jnp.concatenate([spread, pad], axis=0).T
        high = spread.astype(jnp.bfloat16)
        share[0] = high
        share[1] = (spread - high.astype(jnp.float32)).astype(jnp.bfloat16)

    def mix(first_row, last_row):
        rows = returned[first_row:last_row]
        high, low = share[0, :, first_row:last_row], share[1, :, first_row:last_row]
        return dot_f32(high, rows) + dot_f32(low, rows)

    stages = {
        "forward": forward, "pass_on": pass_on, "compute": compute, "down": down,
        "attend": attend, "latents": send_latents, "gather": gather_latents, "relay": relay_latents, "give": give, "weights": weights,
        "settle": settle, "prepare": prepare, "send": send, "gated": gated,
    }
    for stage, at in plan(count, query_t.shape[0]):
        stages[stage](at)

    for k in near + sequence[: half - 2]:
        give_back(k).wait_recv()
    mixed[...] = mix(0, early)
    for k in sequence[half - 2 :]:
        give_back(k).wait_recv()
    settle_extra().wait_recv()
    out_ref[...] = (mixed[...] + mix(early, total_rows)).astype(jnp.bfloat16)
    for copy in (latents_across, latents_beside, latents_relay):
        copy.wait_send()
    near_back = back_send.at[pl.ds(0, half - 1)]
    shares = hidden.at[pl.ds(0, 3 * count // 4)]
    for ref, spot in ((arrived, 0), (near_back, 1), (shares, 2), (three, 3)):
        remote(ref, ref, sent.at[spot], wd_r.at[0], me, other_core).wait_send()


def base_rows(row_count, capacity, count):
    spare = -(-(row_count - capacity) // (count - 1))
    return 16 * -(-spare // 16)


def window_fused(
    queries, latents, block_starts, w_uv, moe_tokens, expert_ids, gate_weights, w_gate, w_up, w_down
):
    queries = jnp.transpose(queries, (1, 2, 0))
    heads, entry_width, query_tokens = queries.shape
    lat_width, value_width = w_uv.shape[1:]
    ways = lax.axis_size("ctx")
    key_count = ways * query_tokens
    token_count, picks = expert_ids.shape
    model_width = moe_tokens.shape[1]
    fan = w_gate.shape[2]
    count = lax.axis_size("exp")
    width = model_width // ways
    capacity = 3 * token_count * picks // (2 * count)
    half = count // 2
    base = base_rows(token_count * picks, capacity, count)
    rest = capacity - base
    share_width = 128 * -(-(half * (capacity + base) + rest) // 128)
    vmem = pl.BlockSpec(memory_space=pltpu.VMEM)
    hbm = pl.BlockSpec(memory_space=pltpu.HBM)
    block = (capacity, width)
    dtype = jnp.bfloat16
    dma = pltpu.SemaphoreType.DMA
    routed, attended = pl.pallas_call(
        functools.partial(window_kernel, count, capacity, base),
        out_shape=(
            jax.ShapeDtypeStruct((token_count, width), dtype),
            jax.ShapeDtypeStruct((heads, query_tokens, value_width), dtype),
        ),
        in_specs=[hbm] * 10,
        out_specs=(vmem, vmem),
        scratch_shapes=[
            pltpu.VMEM((picks, token_count), jnp.int32),
            pltpu.VMEM((picks, token_count), jnp.float32),
            pltpu.VMEM((entry_width, query_tokens), dtype),
            pltpu.VMEM((token_count, model_width), dtype),
            pltpu.SMEM(block_starts.shape, jnp.int32),
            pltpu.VMEM((model_width, 2 * fan), dtype),
            pltpu.VMEM((ways, fan, width), dtype),
            pltpu.VMEM(queries.shape, dtype),
            pltpu.VMEM(w_uv.shape, dtype),
            pltpu.VMEM((ways, entry_width, query_tokens), dtype),
            pltpu.VMEM((key_count, entry_width), dtype),
            pltpu.VMEM((lat_width, key_count), dtype),
            pltpu.VMEM((key_count, query_tokens), jnp.float32),
            pltpu.VMEM((count, token_count), jnp.float32),
            pltpu.VMEM((count, token_count), jnp.float32),
            pltpu.VMEM((half, 2) + block, dtype),
            pltpu.VMEM((half * base + rest, width), dtype),
            pltpu.VMEM((rest, width), dtype),
            pltpu.VMEM((ways, count) + block, dtype),
            pltpu.VMEM((count, ways, capacity, fan), dtype),
            pltpu.VMEM((count,) + block, dtype),
            pltpu.VMEM((half, rest, width), dtype),
            pltpu.VMEM((rest, width), dtype),
            pltpu.VMEM((half * (capacity + base) + rest, width), dtype),
            pltpu.VMEM((2, token_count, share_width), dtype),
            pltpu.VMEM((token_count, width), jnp.float32),
            dma((10,)), dma((3,)), dma((3,)), dma((4,)),
            dma((count, 2)), dma((count,)), dma((count, 2)), dma((count,)),
            dma((count, 3)), dma((1,)), dma((count,)), dma((half, 2)), dma((half,)), dma((1,)),
        ],
        compiler_params=pltpu.CompilerParams(
            collective_id=0, has_side_effects=True, vmem_limit_bytes=40 * 1024 * 1024
        ),
    )(
        *[
            pltpu.with_memory_space_constraint(operand, pltpu.HBM)
            for operand in (
                expert_ids.T, gate_weights.T, latents.T, moe_tokens, block_starts,
                w_gate, w_up, w_down, queries, w_uv,
            )
        ]
    )
    return jnp.transpose(attended, (1, 0, 2)), routed


def shards(
    queries, latents, block_starts, w_uv, moe_tokens, expert_ids, gate_weights, w_gate, w_up, w_down
):
    count = lax.axis_size("exp")
    ways = lax.axis_size("ctx")
    token_count, picks = expert_ids.shape
    capacity = 3 * token_count * picks // (2 * count)
    fits = ways == 4 and count & (count - 1) == 0 and count >= 4 and capacity % 16 == 0
    fits = fits and moe_tokens.shape[1] % (128 * ways) == 0 and block_starts.shape[0] == 8
    base = base_rows(token_count * picks, capacity, count)
    fits = fits and 3 * base == 2 * capacity and count == 8
    fits = fits and picks == 2 and w_gate.shape[2] % 128 == 0
    if fits:
        return window_fused(
            queries, latents, block_starts, w_uv, moe_tokens, expert_ids, gate_weights,
            w_gate, w_up, w_down,
        )
    attended = attention(queries, latents, block_starts, w_uv)
    return attended, routed_plain(moe_tokens, expert_ids, gate_weights, w_gate, w_up, w_down)


def solution(mesh):
    in_specs = (
        P("ctx", "exp", None),
        P("ctx", None),
        P(),
        P("exp", None, None),
        P("exp", None),
        P("exp", None),
        P("exp", None),
        P("exp", None, "ctx"),
        P("exp", None, "ctx"),
        P("exp", "ctx", None),
    )
    out_specs = (P("ctx", "exp", None), P("exp", "ctx"))
    return jax.shard_map(shards, mesh=mesh, in_specs=in_specs, out_specs=out_specs, check_vma=False)
```
